32 devices in a mesh: rows: 32 (over z, y, x, core).
Axes of the slice: x: 2, y: 2, z: 4, core: 2. Of those that a mesh axis runs over, the one named last changes fastest.
Arguments:
- right_side: float32 [524288], P('rows'), may hold values from -24 to 24
- diag_shift: float32 [524288], P('rows'), may hold values from 0.05 to 0.5
- dictionary: float32 [128, 128, 128], replicated, may hold values from -16.5 to 16.5, as said below
- diag_ids: int32 [4096], P('rows'), may hold values from 0 to 127
- diag_gain: float32 [4096], P('rows'), may hold values from 0.3 to 1.5
- cycle_ids: int32 [4096, 2], P('rows'), may hold values from 0 to 127, as said below
- cycle_weights: float32 [4096, 2], P('rows'), may hold values from 0.3 to 1.5, as said below
- link_rows: int32 [32, 5, 64], P('rows'), may hold values from 0 to 127, as said below
- link_ids: int32 [32, 5, 64], P('rows'), may hold values from 0 to 127, as said below
- link_weights: float32 [32, 5, 64], P('rows'), may hold values from 0.3 to 1.5, as said below
Outputs:
- solution_field: float32 [524288], P('rows')
- residual: float32 [524288], P('rows')
The draws below stay inside these ranges and needn't reach their ends.
Inputs may be any that keep to these rules, and one draw needn't show every extreme that they name: `dictionary`: every block is symmetric positive definite. cycle_ids[i,1] equals cycle_ids[(i+1) mod 4096,0]. cycle_weights[i,1] equals cycle_weights[(i+1) mod 4096,0]. `link_rows`: for each device and level the 64 entries are distinct. `link_ids`: devices d and d XOR 2^b at level m (b = log2 of the number of devices - 1 - m) hold the same entries in the same order. `link_weights`: devices d and d XOR 2^b at level m (b = log2 of the number of devices - 1 - m) hold the same entries in the same order.
All inputs are finite; a program needn't handle non-finite values.
Results may differ from the reference program's by a relative error of at most 0.0003.
Values sent between devices are 32-bit elements; how exact they have to be, the bound alone decides.
No kernel may reach another device: no remote copies, remote signals or barrier semaphores. Data moves between devices by JAX's collectives and lax.ppermute only.
A program may use at most 128 MiB of HBM per device.

```python
import math
import jax
import jax.numpy as jnp
from jax import lax

BS = 128
DICT = 128
NB_DEV = 128
ITERS = 4
LEVELS = 5
HALF = 64
BLOCKS = 4096


def draw_right_side(key, part):
    length_all = BLOCKS * BS
    rising = 1.0 + 2.0 * jnp.arange(length_all, dtype=jnp.float32) / length_all
    normal_part = jnp.clip(jax.random.normal(key, (length_all,), jnp.float32), -4.0, 4.0)
    return 2.0 * rising * normal_part


def draw_dictionary(key, part):
    factor = jnp.clip(jax.random.normal(jax.random.fold_in(key, 13), (DICT, BS, BS), jnp.float32), -4.0, 4.0)
    gram_blocks = jnp.einsum('kij,klj->kil', factor, factor, precision=jax.lax.Precision.HIGHEST) / BS
    return gram_blocks + 0.5 * jnp.eye(BS, dtype=jnp.float32)


def cycle_pair(values):
    return jnp.stack([jnp.roll(values, 1), values], axis=1)


def draw_cycle_ids(key, part):
    drawn = jax.random.randint(jax.random.fold_in(key, 21), (BLOCKS,), 0, DICT, jnp.int32)
    return cycle_pair(drawn)


def weight_values(key, shape):
    return jnp.exp(jax.random.uniform(key, shape, jnp.float32, math.log(0.3), math.log(1.5)))


def draw_cycle_weights(key, part):
    return cycle_pair(weight_values(jax.random.fold_in(key, 22), (BLOCKS,)))


def mirror(drawn):
    devices = BLOCKS // NB_DEV
    bit_count = devices.bit_length() - 1
    owners = jnp.arange(devices, dtype=jnp.int32)
    stacked = []
    for level_idx in range(LEVELS):
        partner = jnp.bitwise_xor(owners, jnp.int32(1 << bit_count - 1 - level_idx))
        lowest = jnp.minimum(owners, partner)
        stacked.append(drawn[lowest, level_idx])
    return jnp.stack(stacked, axis=1)


def draw_link_rows(key, part):
    devices = BLOCKS // NB_DEV
    subkeys = jax.random.split(jax.random.fold_in(key, 31), devices * LEVELS)
    orders = jax.vmap(lambda subkey: jax.random.permutation(subkey, NB_DEV))(subkeys)
    return orders[:, :HALF].reshape(devices, LEVELS, HALF).astype(jnp.int32)


def draw_link_ids(key, part):
    devices = BLOCKS // NB_DEV
    drawn = jax.random.randint(jax.random.fold_in(key, 32), (devices, LEVELS, HALF), 0, DICT, jnp.int32)
    return mirror(drawn)


def draw_link_weights(key, part):
    devices = BLOCKS // NB_DEV
    return mirror(weight_values(jax.random.fold_in(key, 33), (devices, LEVELS, HALF)))


def set_ends(entries, key, least, top_value):
    shape = entries.shape
    spot = [jax.random.randint(jax.random.fold_in(key, axis), (), 0, shape[axis]) for axis in range(len(shape))]
    entries = entries.at[tuple(spot)].set(least)
    longest = shape.index(max(shape))
    spot[longest] = (spot[longest] + 1) % shape[longest]
    return entries.at[tuple(spot)].set(top_value)


def block_scale(key, dims, shards, smallest, high):
    def one(axis_at, parts):
        steps = jax.random.uniform(jax.random.fold_in(jax.random.fold_in(key, 6), axis_at), (parts,), jnp.float32, smallest / len(shards), high / len(shards))
        return jnp.repeat(jnp.exp(steps), dims[axis_at] // parts).reshape((-1,) + (1,) * (len(dims) - axis_at - 1))

    level = one(*shards[0])
    for cut in shards[1:]:
        level = level * one(*cut)
    return level


def setup_inputs(seed: int = 0) -> dict:
    key_list = jax.random.split(jax.random.key(seed), 11)
    right_side = draw_right_side(jax.random.fold_in(key_list[10], 71), 0)
    diag_shift = jnp.clip(jnp.exp(math.log(0.5) - 2.3025851 * jax.random.uniform(key_list[1], (BLOCKS * BS,), jnp.float32) ** block_scale(key_list[1], (BLOCKS * BS,), ((0, 32),), -0.2, 0.2)), 0.05, 0.5)
    dictionary = draw_dictionary(jax.random.fold_in(key_list[10], 71), 0)
    diag_ids = set_ends(jax.random.randint(key_list[3], (BLOCKS,), 0, DICT), jax.random.fold_in(key_list[3], 1), 0, DICT - 1).astype(jnp.int32)
    diag_gain = jnp.clip(jnp.exp(math.log(1.5) - 1.60943787 * jax.random.uniform(key_list[4], (BLOCKS,), jnp.float32) ** block_scale(key_list[4], (BLOCKS,), ((0, 32),), -0.2, 0.2)), 0.3, 1.5)
    cycle_ids = draw_cycle_ids(jax.random.fold_in(key_list[10], 71), 0)
    cycle_weights = draw_cycle_weights(jax.random.fold_in(key_list[10], 71), 0)
    link_rows = draw_link_rows(jax.random.fold_in(key_list[10], 71), 0)
    link_ids = draw_link_ids(jax.random.fold_in(key_list[10], 71), 0)
    link_weights = draw_link_weights(jax.random.fold_in(key_list[10], 71), 0)
    return dict(right_side=right_side, diag_shift=diag_shift, dictionary=dictionary, diag_ids=diag_ids, diag_gain=diag_gain, cycle_ids=cycle_ids, cycle_weights=cycle_weights, link_rows=link_rows, link_ids=link_ids, link_weights=link_weights)


def batched(mats, vectors):
    return jnp.einsum('nij,nj->ni', mats, vectors, precision=lax.Precision.HIGHEST)


def apply_operator(vector, diag_shift, dictionary, diag_ids, diag_gain, cycle_ids, cycle_weights, link_rows, link_ids, link_weights):
    devices = BLOCKS // NB_DEV
    bit_count = devices.bit_length() - 1
    flat = vector.reshape(BLOCKS, BS)
    lower_blocks = jnp.roll(flat, 1, axis=0).reshape(devices, NB_DEV, BS)
    upper_blocks = jnp.roll(flat, -1, axis=0).reshape(devices, NB_DEV, BS)
    grouped = flat.reshape(devices, NB_DEV, BS)
    owners = jnp.arange(devices, dtype=jnp.int32)
    differences = []
    for level_idx in range(LEVELS):
        partner = jnp.bitwise_xor(owners, jnp.int32(1 << (bit_count - 1 - level_idx)))
        own_part = grouped[owners[:, None], link_rows[:, level_idx]]
        remote = grouped[partner[:, None], link_rows[partner, level_idx]]
        differences.append(own_part - remote)
    link_diff = jnp.stack(differences, axis=1)

    def one_device(pieces):
        block_vec, below_vec, above_vec, shifts, dids, dgain, rids, rweights, lrows, lids, lweights, ldiff = pieces
        diag_mats = dictionary[dids] * dgain[:, None, None]
        lower_mats = dictionary[rids[:, 0]] * rweights[:, 0, None, None]
        upper_mats = dictionary[rids[:, 1]] * rweights[:, 1, None, None]
        result = shifts * block_vec + batched(diag_mats, block_vec)
        result = result + batched(lower_mats, block_vec - below_vec) + batched(upper_mats, block_vec - above_vec)
        link_mats = dictionary[lids] * lweights[:, :, None, None]
        products = jnp.einsum('lhij,lhj->lhi', link_mats, ldiff, precision=lax.Precision.HIGHEST)
        selector = (lrows[:, :, None] == jnp.arange(NB_DEV, dtype=jnp.int32)).astype(jnp.float32)
        return result + jnp.einsum('lhn,lhi->ni', selector, products, precision=lax.Precision.HIGHEST)

    results = lax.map(one_device, (grouped, lower_blocks, upper_blocks, diag_shift.reshape(devices, NB_DEV, BS),
                                   diag_ids.reshape(devices, NB_DEV), diag_gain.reshape(devices, NB_DEV),
                                   cycle_ids.reshape(devices, NB_DEV, 2), cycle_weights.reshape(devices, NB_DEV, 2),
                                   link_rows, link_ids, link_weights, link_diff))
    return results.reshape(-1)


def reference(right_side, diag_shift, dictionary, diag_ids, diag_gain, cycle_ids, cycle_weights, link_rows, link_ids, link_weights):
    def operate(vector):
        return apply_operator(vector, diag_shift, dictionary, diag_ids, diag_gain, cycle_ids, cycle_weights, link_rows, link_ids, link_weights)

    solution_field = jnp.zeros_like(right_side)
    residual = right_side
    image_vec = operate(residual)
    norm_now = jnp.sum(residual * residual)
    product = jnp.sum(residual * image_vec)
    step_size = norm_now / product
    direction, image_dir = residual, image_vec
    for iteration in range(ITERS):
        solution_field = solution_field + step_size * direction
        residual = residual - step_size * image_dir
        if iteration + 1 < ITERS:
            image_vec = operate(residual)
            norm_next = jnp.sum(residual * residual)
            product = jnp.sum(residual * image_vec)
            beta_ratio = norm_next / norm_now
            step_size = norm_next / (product - beta_ratio * norm_next / step_size)
            direction = residual + beta_ratio * direction
            image_dir = image_vec + beta_ratio * image_dir
            norm_now = norm_next
    return solution_field, residual
```

```python
import functools

import jax
import jax.numpy as jnp
from jax import lax
from jax.experimental import pallas as pl
from jax.experimental.pallas import tpu as pltpu
from jax.sharding import PartitionSpec as P


ITERS = 4
SLOT = 8
GROUP = 128
SHIFT = 1.5
F32 = jnp.float32
BF16 = jnp.bfloat16


def dot(a, b, dims=((1,), (0,))):
    return lax.dot_general(a, b, (dims, ((), ())), preferred_element_type=F32)


NT = ((1,), (1,))
TN = ((0,), (0,))


def halves(x):
    high = x.astype(BF16).astype(F32)
    return high, x - high


def halves_wide(x):
    high, low = halves(x)
    return jnp.concatenate([high, low], axis=1).astype(BF16)


def iota(shape, dim):
    return lax.broadcasted_iota(jnp.int32, shape, dim)


def onehot(cond):
    return jnp.where(cond, 1.0, 0.0)


def send_blocks(select_ref, block_vec, send_refs, edge_ref, merged):
    nb = block_vec.shape[0]
    edge = jnp.concatenate([block_vec[0:1], block_vec[nb - 1 :]], axis=0)
    edge = jnp.concatenate([edge, jnp.zeros((6, block_vec.shape[1]), F32)], axis=0)
    wide = halves_wide(block_vec)
    picked = dot(select_ref[...], wide)
    width = block_vec.shape[1]
    picked = picked[:, :width] + picked[:, width:]
    half = picked.shape[0] // len(send_refs)
    for level, ref in enumerate(send_refs):
        ref[0:half, :] = picked[level * half : (level + 1) * half]
        if level == merged:
            ref[half : half + 8, :] = edge
    edge_ref[...] = edge


def prepare(
    parity_ref, dict_hbm, vec_ref, ids_ref, weights_ref, rows_ref,
    *refs, nb, levels, half, merged, groups, sources,
):
    sends, (edge_ref, select_ref, gather_ref, scatter_ref, wide_ref, table_ref, scale_ref) = (
        refs[:levels], refs[levels : levels + 7],
    )
    dict_vmem, sems = refs[levels + 7 :]
    blocks, width, _ = dict_hbm.shape
    parts = sems.shape[0]
    per = blocks // parts

    def load(part):
        span = pl.ds(part * per, per)
        return pltpu.make_async_copy(dict_hbm.at[span], dict_vmem.at[span], sems.at[part])

    for part in range(parts):
        load(part).start()

    entries = ids_ref.shape[1]
    ids = ids_ref[...]
    weights = weights_ref[...]
    rows = rows_ref[...]
    lane = iota((1, entries), 1)
    links = levels * half
    tail = 2 * nb + links
    is_lower = (lane >= nb) & (lane < 2 * nb)
    is_link = (lane >= 2 * nb) & (lane < tail)
    is_tail = lane == tail
    even = parity_ref[0] == 0
    edge_base = nb + links
    before = jnp.where(even, edge_base + 9, edge_base + 1)
    after = jnp.where(even, edge_base, edge_base + 8)
    plus = jnp.where(lane < nb, lane, jnp.where(is_lower, lane - nb, jnp.where(is_link, rows, jnp.where(is_tail, nb - 1, -1))))
    minus = jnp.where(is_lower & (lane > nb), lane - nb - 1, -1)
    away = jnp.where(
        is_lower,
        jnp.where(lane > nb, lane - nb - 1, before),
        jnp.where(is_link, lane - nb, jnp.where(is_tail, after, -1)),
    )

    row_iota = iota((nb, entries), 0)
    target = onehot(row_iota == plus)
    eye = onehot(iota((nb, nb), 0) == iota((nb, nb), 1)).astype(BF16)
    select_ref[...] = dot(target[:, 2 * nb : tail].astype(BF16), eye, TN).astype(BF16)
    send_blocks(select_ref, vec_ref[...], sends, edge_ref, merged)

    member = onehot(iota((blocks, entries), 0) == ids)
    earlier = onehot(iota((entries, entries), 0) < iota((entries, entries), 1)).astype(BF16)
    ahead = dot(member.astype(BF16), earlier)
    rank = jnp.sum(member * ahead, axis=0, keepdims=True)
    count = jnp.sum(member, axis=1, keepdims=True)
    more = jnp.maximum(jnp.floor((count - 1.0) * (1.0 / SLOT)), 0.0)
    before_block = onehot(iota((blocks, blocks), 1) < iota((blocks, blocks), 0)).astype(BF16)
    more_wide = jnp.broadcast_to(more, (blocks, 128))
    base = dot(before_block, more_wide.astype(BF16))
    base_entry = jnp.sum(member * base[:, 0:1], axis=0, keepdims=True)
    chunk = jnp.floor(rank * (1.0 / SLOT))
    place = rank - SLOT * chunk
    idf = ids.astype(F32)
    slot = jnp.where(
        chunk == 0.0,
        idf * SLOT + place,
        (blocks + base_entry + chunk - 1.0) * SLOT + place,
    )
    slot = jnp.where(ids >= 0, slot, -1.0).astype(jnp.int32)

    chunk_lane = iota((blocks, 128), 1).astype(F32)
    owner = (chunk_lane >= base) & (chunk_lane < base + more_wide)
    block_id = iota((blocks, 128), 0).astype(F32)
    table = jnp.sum(jnp.where(owner, block_id, 0.0), axis=0, keepdims=True)
    total = jnp.sum(more_wide, axis=0, keepdims=True)
    table_ref[...] = jnp.where(iota((1, 128), 1) == 127, total, table).astype(jnp.int32)

    source_iota = iota((sources, entries), 0)
    source = (onehot(source_iota == plus) - onehot(source_iota == away)).astype(BF16)
    signed = target - onehot(row_iota == minus)
    high, low = halves(weights)
    signed = jnp.concatenate([signed * high, signed * low], axis=0).astype(BF16)
    for group in range(groups):
        here = onehot(iota((GROUP, entries), 0) + group * GROUP == slot).astype(BF16)
        gather_ref[group * GROUP : (group + 1) * GROUP, :] = dot(here, source, NT).astype(BF16)
        scatter_ref[:, group * GROUP : (group + 1) * GROUP] = dot(signed, here, NT).astype(BF16)

    def split_block(k, acc):
        block = dict_vmem[k]
        block_high = block.astype(BF16)
        wide_ref[k, :, 0:width] = block_high
        wide_ref[k, :, width : 2 * width] = (block - block_high.astype(F32)).astype(BF16)
        return acc + block

    acc = jnp.zeros((width, width), F32)
    for part in range(parts):
        load(part).wait()
        acc = lax.fori_loop(part * per, (part + 1) * per, split_block, acc, unroll=4)
    diagonal = onehot(iota((width, width), 0) == iota((width, width), 1))
    trace = jnp.sum(jnp.sum(acc * diagonal, axis=0, keepdims=True), axis=1, keepdims=True)
    scale = 1.0 / (trace * (4.25 / (blocks * width)) + 0.5)
    scale_ref[...] = jnp.broadcast_to(scale, (1, 128))


def apply_operator(
    table_ref, vec_ref, shift_ref, scale_ref, recv_refs, edge_ref,
    gather_ref, scatter_ref, wide_ref, scratch, *, half, merged,
):
    sources_ref, lhs_ref, prod_ref = scratch
    nb, width = vec_ref.shape
    blocks = wide_ref.shape[0]
    chunks = GROUP // SLOT
    levels = len(recv_refs)
    vec = vec_ref[...]
    sources_ref[0:nb, :] = halves_wide(vec)
    for level, ref in enumerate(recv_refs):
        start = nb + level * half
        sources_ref[start : start + half, :] = halves_wide(ref[0:half, :])
    start = nb + levels * half
    mine = recv_refs[merged][half : half + 8, :] if merged >= 0 else edge_ref[8:16, :]
    sources_ref[start : start + 16, :] = halves_wide(jnp.concatenate([mine, edge_ref[0:8, :]], axis=0))
    rest = sources_ref.shape[0] - start - 16
    if rest:
        sources_ref[start + 16 :, :] = jnp.zeros((rest, 2 * width), BF16)

    def stage(picked):
        picked = picked[:, :width] + picked[:, width:]
        high, low = halves(picked)
        for chunk in range(chunks):
            span = slice(chunk * SLOT, (chunk + 1) * SLOT)
            yield jnp.concatenate([high[span], low[span]], axis=0).astype(BF16)

    def product(lhs, block):
        wide = dot(lhs, block)
        return wide[:SLOT, :width] + wide[:SLOT, width:] + wide[SLOT:, :width]

    main = blocks * SLOT
    for group in range(main // GROUP):
        span = slice(group * GROUP, (group + 1) * GROUP)
        lhs = list(stage(dot(gather_ref[span, :], sources_ref[...])))
        prods = [product(lhs[c], wide_ref[group * chunks + c]) for c in range(chunks)]
        prod_ref[span, :] = halves_wide(jnp.concatenate(prods, axis=0))
    total = dot(scatter_ref[:, 0:main], prod_ref[0:main, :])
    out = total[:nb, :width] + total[:nb, width:] + total[nb:, :width]

    def further(group, out):
        span = pl.ds(pl.multiple_of(main + group * GROUP, GROUP), GROUP)
        picked = dot(gather_ref[span, :], sources_ref[...])
        lhs = list(stage(picked))
        prods = [product(lhs[c], wide_ref[table_ref[0, group * chunks + c]]) for c in range(chunks)]
        part = dot(scatter_ref[:, span], halves_wide(jnp.concatenate(prods, axis=0)))
        return out + part[:nb, :width] + part[:nb, width:] + part[nb:, :width]

    out = lax.fori_loop(0, (table_ref[0, 127] + chunks - 1) // chunks, further, out)
    return (shift_ref[...] * vec + out) * scale_ref[...] - SHIFT * vec


def step_kernel(*refs, levels, half, merged):
    table_ref, vec_ref, shift_ref, scale_ref, *rest = refs
    recv_refs, rest = rest[:levels], rest[levels:]
    edge_ref, select_ref, gather_ref, scatter_ref, wide_ref, next_ref, *rest = rest
    sends, (send_edge_ref, *scratch) = rest[:levels], rest[levels:]
    following = apply_operator(
        table_ref, vec_ref, shift_ref, scale_ref, recv_refs, edge_ref,
        gather_ref, scatter_ref, wide_ref, scratch, half=half, merged=merged,
    )
    next_ref[...] = following
    send_blocks(select_ref, following, sends, send_edge_ref, merged)


PAIRS = [(i, j) for i in range(ITERS + 1) for j in range(i, ITERS + 1)]


def last_kernel(*refs, levels, half, merged):
    table_ref, vec_ref, shift_ref, scale_ref, *rest = refs
    recv_refs, rest = rest[:levels], rest[levels:]
    edge_ref, gather_ref, scatter_ref, wide_ref, *rest = rest
    older, (next_ref, sums_ref, *scratch) = rest[: ITERS - 1], rest[ITERS - 1 :]
    following = apply_operator(
        table_ref, vec_ref, shift_ref, scale_ref, recv_refs, edge_ref,
        gather_ref, scatter_ref, wide_ref, scratch, half=half, merged=merged,
    )
    next_ref[...] = following
    basis = [ref[...] for ref in older] + [vec_ref[...], following]
    sums = [jnp.sum(basis[i] * basis[j], axis=0, keepdims=True) for i, j in PAIRS]
    sums = jnp.concatenate(sums + [jnp.zeros((1, sums[0].shape[1]), F32)] * (-len(PAIRS) % 8), axis=0)
    column = jnp.sum(sums, axis=1, keepdims=True)
    at = iota((column.shape[0], 128), 0) == iota((column.shape[0], 128), 1)
    row = jnp.sum(jnp.where(at, column, 0.0), axis=0, keepdims=True)
    sums_ref[...] = jnp.broadcast_to(row, sums_ref.shape)


def finish(sums_ref, scale_ref, *refs):
    basis_refs, (solution_ref, residual_ref) = refs[: ITERS + 1], refs[ITERS + 1 :]
    row = jnp.sum(sums_ref[...], axis=0, keepdims=True)
    lane = iota(row.shape, 1)
    gram = {}
    for index, (i, j) in enumerate(PAIRS):
        entry = jnp.sum(jnp.where(lane == index, row, 0.0), axis=1, keepdims=True)
        gram[i, j] = gram[j, i] = entry
    unscale = 1.0 / scale_ref[0:1, 0:1]
    one = jnp.ones((1, 1), F32)

    def image_of(coefs):
        out = [None] * (len(coefs) + 1)
        for k, c in enumerate(coefs):
            up = c * unscale
            out[k] = SHIFT * up if out[k] is None else out[k] + SHIFT * up
            out[k + 1] = up
        return out

    def inner(a, b):
        rows = []
        for i, x in enumerate(a):
            rows.append(x * sum(gram[i, j] * y for j, y in enumerate(b)))
        return sum(rows)

    def plus(a, factor, b):
        out = list(a) + [None] * (len(b) - len(a))
        for k, y in enumerate(b):
            out[k] = factor * y if out[k] is None else out[k] + factor * y
        return out

    residual = [one]
    field = []
    image = image_of(residual)
    norm = inner(residual, residual)
    step = norm / inner(residual, image)
    direction, along = residual, image
    for k in range(ITERS):
        field = plus(field, step, direction)
        residual = plus(residual, -step, along)
        if k + 1 < ITERS:
            image = image_of(residual)
            following = inner(residual, residual)
            product = inner(residual, image)
            ratio = following / norm
            step = following / (product - ratio * following / step)
            direction = plus(residual, ratio, direction)
            along = plus(image, ratio, along)
            norm = following
    basis = [ref[...] for ref in basis_refs]
    solution_ref[...] = sum(c * v for c, v in zip(field, basis))
    residual_ref[...] = sum(c * v for c, v in zip(residual, basis))


def params(mib):
    return pltpu.CompilerParams(vmem_limit_bytes=mib * 1024 * 1024)


def vmem(count):
    return [pl.BlockSpec(memory_space=pltpu.VMEM)] * count


def shape(dims, dtype=F32):
    return jax.ShapeDtypeStruct(dims, dtype)


def per_device(
    right_side, diag_shift, dictionary, diag_ids, diag_gain, cycle_ids, cycle_weights,
    link_rows, link_ids, link_weights, *, devices,
):
    nb = diag_ids.shape[0]
    blocks, width, _ = dictionary.shape
    _, levels, half = link_rows.shape
    bits = devices.bit_length() - 1
    masks = [2 ** (bits - 1 - level) for level in range(levels)]
    merged = masks.index(1) if 1 in masks else -1
    links = levels * half
    used = 2 * nb + links + 1
    entries = -(-used // 128) * 128
    sources = -(-(nb + links + 16) // 128) * 128
    extra = -(-(used // SLOT) // (GROUP // SLOT))
    groups = blocks * SLOT // GROUP + extra

    pad = entries - used
    ids = jnp.concatenate(
        [diag_ids, cycle_ids[:, 0], link_ids.reshape(-1), cycle_ids[-1:, 1], jnp.full((pad,), -1, jnp.int32)]
    )[None]
    weights = jnp.concatenate(
        [diag_gain, cycle_weights[:, 0], link_weights.reshape(-1), cycle_weights[-1:, 1], jnp.zeros((pad,), F32)]
    )[None]
    rows = jnp.pad(link_rows.reshape(1, -1), ((0, 0), (2 * nb, entries - 2 * nb - links)))
    parity = (lax.axis_index("rows") % 2).astype(jnp.int32)[None]
    first = right_side.reshape(nb, width)
    shifts = diag_shift.reshape(nb, width)

    send_shapes = [shape((half + 8 * (level == merged), width)) for level in range(levels)]
    edge_shape = shape((8, width))
    outs = pl.pallas_call(
        functools.partial(
            prepare, nb=nb, levels=levels, half=half, merged=merged, groups=groups, sources=sources
        ),
        out_shape=send_shapes
        + [
            edge_shape,
            shape((links, nb), BF16),
            shape((groups * GROUP, sources), BF16),
            shape((2 * nb, groups * GROUP), BF16),
            shape((blocks, width, 2 * width), BF16),
            shape((1, 128), jnp.int32),
            shape((1, 128)),
        ],
        in_specs=[pl.BlockSpec(memory_space=pltpu.SMEM), pl.BlockSpec(memory_space=pl.ANY)] + vmem(4),
        out_specs=vmem(levels + 7),
        scratch_shapes=[pltpu.VMEM((blocks, width, width), F32), pltpu.SemaphoreType.DMA((4,))],
        compiler_params=params(40),
        name="prepare",
    )(parity, dictionary, first, ids, weights, rows)
    sends, (edge, select, gather, scatter, wide, table, scale) = outs[:levels], outs[levels:]

    def exchange(sends, edge):
        near = [(i, i ^ 1) for i in range(devices)]
        far = [(i, (i + 1) % devices if i % 2 else (i - 1) % devices) for i in range(devices)]
        got = [
            lax.ppermute(sends[level], "rows", [(i, i ^ masks[level]) for i in range(devices)])
            for level in range(levels)
        ]
        edges = lax.ppermute(edge, "rows", far)
        if merged < 0:
            edges = jnp.concatenate([edges, lax.ppermute(edge, "rows", near)], axis=0)
        return got, edges

    scratch = [
        pltpu.VMEM((sources, 2 * width), BF16),
        pltpu.VMEM((8, 128), BF16),
        pltpu.VMEM((blocks * SLOT, 2 * width), BF16),
    ]
    smem = [pl.BlockSpec(memory_space=pltpu.SMEM)]
    basis = [first]
    for k in range(ITERS):
        got, edges = exchange(sends, edge)
        common = dict(levels=levels, half=half, merged=merged)
        if k + 1 < ITERS:
            following, *outs = pl.pallas_call(
                functools.partial(step_kernel, **common),
                out_shape=[shape((nb, width))] + send_shapes + [edge_shape],
                in_specs=smem + vmem(8 + levels),
                out_specs=vmem(levels + 2),
                scratch_shapes=scratch,
                compiler_params=params(24),
                name="step",
            )(table, basis[-1], shifts, scale, *got, edges, select, gather, scatter, wide)
            sends, edge = outs[:levels], outs[levels]
        else:
            following, sums = pl.pallas_call(
                functools.partial(last_kernel, **common),
                out_shape=[shape((nb, width)), shape((devices, 128))],
                in_specs=smem + vmem(7 + levels + ITERS - 1),
                out_specs=vmem(2),
                scratch_shapes=scratch,
                compiler_params=params(24),
                name="last",
            )(table, basis[-1], shifts, scale, *got, edges, gather, scatter, wide, *basis[:-1])
        basis.append(following)
    sums = lax.all_to_all(sums, "rows", 0, 0, tiled=True)
    field, residual = pl.pallas_call(
        finish,
        out_shape=[shape((nb, width))] * 2,
        in_specs=vmem(2 + len(basis)),
        out_specs=vmem(2),
        compiler_params=params(8),
        name="finish",
    )(sums, scale, *basis)
    return field.reshape(-1), residual.reshape(-1)


def solution(mesh):
    placed = (
        P("rows"), P("rows"), P(), P("rows"), P("rows"), P("rows", None), P("rows", None),
        P("rows", None, None), P("rows", None, None), P("rows", None, None),
    )
    return jax.shard_map(
        functools.partial(per_device, devices=mesh.shape["rows"]),
        mesh=mesh, in_specs=placed, out_specs=(P("rows"), P("rows")), check_vma=False,
    )
```

```python
import functools

import jax
import jax.numpy as jnp
from jax import lax
from jax.experimental import pallas as pl
from jax.experimental.pallas import tpu as pltpu
from jax.sharding import PartitionSpec as P


ITERS = 4
SLOT = 8
GROUP = 128
SHIFT = 1.5
F32 = jnp.float32
BF16 = jnp.bfloat16


def dot(a, b, dims=((1,), (0,))):
    return lax.dot_general(a, b, (dims, ((), ())), preferred_element_type=F32)


NT = ((1,), (1,))
TN = ((0,), (0,))


def halves(x):
    high = x.astype(BF16).astype(F32)
    return high, x - high


def halves_wide(x):
    high, low = halves(x)
    return jnp.concatenate([high, low], axis=1).astype(BF16)


def iota(shape, dim):
    return lax.broadcasted_iota(jnp.int32, shape, dim)


def onehot(cond):
    return jnp.where(cond, 1.0, 0.0)


def send_blocks(select_ref, block_vec, send_refs, edge_ref, merged):
    nb = block_vec.shape[0]
    edge = jnp.concatenate([block_vec[0:1], block_vec[nb - 1 :]], axis=0)
    edge = jnp.concatenate([edge, jnp.zeros((6, block_vec.shape[1]), F32)], axis=0)
    wide = halves_wide(block_vec)
    picked = dot(select_ref[...], wide)
    width = block_vec.shape[1]
    picked = picked[:, :width] + picked[:, width:]
    half = picked.shape[0] // len(send_refs)
    for level, ref in enumerate(send_refs):
        ref[0:half, :] = picked[level * half : (level + 1) * half]
        if level == merged:
            ref[half : half + 8, :] = edge
    edge_ref[...] = edge


def prepare(
    parity_ref, dict_hbm, vec_hbm, own_ids_ref, own_weights_ref, near_ids_ref, near_weights_ref,
    link_rows_ref, link_ids_ref, link_weights_ref,
    *refs, nb, levels, half, merged, groups, sure, entries, sources,
):
    sends, (edge_ref, select_ref, gather_ref, scatter_ref, wide_ref, table_ref, scale_ref) = (
        refs[:levels], refs[levels : levels + 7],
    )
    dict_vmem, vec_vmem, here_ref, source_ref, signed_ref, sems = refs[levels + 7 :]
    blocks, width, _ = dict_hbm.shape
    parts = sems.shape[0] - 1
    per = blocks // parts

    def load(part):
        span = pl.ds(part * per, per)
        return pltpu.make_async_copy(dict_hbm.at[span], dict_vmem.at[span], sems.at[part])

    load_vec = pltpu.make_async_copy(vec_hbm, vec_vmem, sems.at[parts])
    load_vec.start()
    for part in range(parts):
        load(part).start()

    links = levels * half
    tail = 2 * nb + links
    pad = entries - tail - 1

    def row_of(own, near, link, last):
        pieces = [own, near] + [link[level] for level in range(levels)]
        return jnp.concatenate(pieces + [last, jnp.zeros((1, pad), last.dtype)], axis=1)

    lane = iota((1, entries), 1)
    ids = row_of(own_ids_ref[...], near_ids_ref[0:1, :], link_ids_ref, near_ids_ref[1:2, nb - 1 : nb])
    ids = jnp.where(lane > tail, -1, ids)
    weights = row_of(
        own_weights_ref[...], near_weights_ref[0:1, :], link_weights_ref, near_weights_ref[1:2, nb - 1 : nb]
    )
    zeros = jnp.zeros((1, nb), jnp.int32)
    rows = row_of(zeros, zeros, link_rows_ref, zeros[:, 0:1])
    is_lower = (lane >= nb) & (lane < 2 * nb)
    is_link = (lane >= 2 * nb) & (lane < tail)
    is_tail = lane == tail
    even = parity_ref[0] == 0
    edge_base = nb + links
    before = jnp.where(even, edge_base + 9, edge_base + 1)
    after = jnp.where(even, edge_base, edge_base + 8)
    plus = jnp.where(is_link, rows, jnp.where(is_tail, nb - 1, -1))
    plus = jnp.where(lane < nb, lane, jnp.where(is_lower, lane - nb, plus))
    minus = jnp.where(is_lower & (lane > nb), lane - nb - 1, -1)
    away = jnp.where(is_link, lane - nb, jnp.where(is_tail, after, -1))
    away = jnp.where(is_lower, jnp.where(lane > nb, lane - nb - 1, before), away)

    member = onehot(iota((blocks, entries), 0) == ids)
    earlier = onehot(iota((entries, entries), 0) < iota((entries, entries), 1)).astype(BF16)
    ahead = dot(member.astype(BF16), earlier)
    rank = jnp.sum(member * ahead, axis=0, keepdims=True)
    count = jnp.sum(member, axis=1, keepdims=True)
    more = jnp.maximum(jnp.floor((count - 1.0) * (1.0 / SLOT)), 0.0)
    before_block = onehot(iota((blocks, blocks), 1) < iota((blocks, blocks), 0)).astype(BF16)
    more_wide = jnp.broadcast_to(more, (blocks, 128))
    base = dot(before_block, more_wide.astype(BF16))
    base_entry = jnp.sum(member * base[:, 0:1], axis=0, keepdims=True)
    chunk = jnp.floor(rank * (1.0 / SLOT))
    place = rank - SLOT * chunk
    idf = ids.astype(F32)
    slot = jnp.where(
        chunk == 0.0,
        idf * SLOT + place,
        (blocks + base_entry + chunk - 1.0) * SLOT + place,
    )
    slot = jnp.where(ids >= 0, slot, -1.0).astype(jnp.int32)

    chunk_lane = iota((blocks, 128), 1).astype(F32)
    owner = (chunk_lane >= base) & (chunk_lane < base + more_wide)
    block_id = iota((blocks, 128), 0).astype(F32)
    table = jnp.sum(jnp.where(owner, block_id, 0.0), axis=0, keepdims=True)
    total = jnp.sum(more_wide, axis=0, keepdims=True)
    table_ref[...] = jnp.where(iota((1, 128), 1) == 127, total, table).astype(jnp.int32)

    row_iota = iota((nb, entries), 0)
    target = onehot(row_iota == plus)
    source_iota = iota((sources, entries), 0)
    source_ref[...] = (onehot(source_iota == plus) - onehot(source_iota == away)).astype(BF16)
    signed = target - onehot(row_iota == minus)
    high, low = halves(weights)
    signed_ref[...] = jnp.concatenate([signed * high, signed * low], axis=0).astype(BF16)
    span = sure * GROUP
    here_ref[...] = onehot(iota((span, entries), 0) == slot).astype(BF16)
    gather_ref[0:span, :] = dot(here_ref[...], source_ref[...], NT).astype(BF16)
    scatter_ref[:, 0:span] = dot(signed_ref[...], here_ref[...], NT).astype(BF16)
    used_chunks = jnp.sum(more).astype(jnp.int32)
    chunks = GROUP // SLOT
    for group in range(sure, groups):

        @pl.when(used_chunks > (group - blocks * SLOT // GROUP) * chunks)
        def _(group=group):
            at = slice(group * GROUP, (group + 1) * GROUP)
            here = onehot(iota((GROUP, entries), 0) + group * GROUP == slot).astype(BF16)
            gather_ref[at, :] = dot(here, source_ref[...], NT).astype(BF16)
            scatter_ref[:, at] = dot(signed_ref[...], here, NT).astype(BF16)

    eye = onehot(iota((nb, nb), 0) == iota((nb, nb), 1)).astype(BF16)
    select_ref[...] = dot(target[:, 2 * nb : tail].astype(BF16), eye, TN).astype(BF16)
    load_vec.wait()
    send_blocks(select_ref, vec_vmem[...], sends, edge_ref, merged)

    def split_block(k, acc):
        block = dict_vmem[k]
        block_high = block.astype(BF16)
        wide_ref[k, :, 0:width] = block_high
        wide_ref[k, :, width : 2 * width] = (block - block_high.astype(F32)).astype(BF16)
        return acc + block

    acc = jnp.zeros((width, width), F32)
    for part in range(parts):
        load(part).wait()
        acc = lax.fori_loop(part * per, (part + 1) * per, split_block, acc, unroll=4)
    diagonal = onehot(iota((width, width), 0) == iota((width, width), 1))
    trace = jnp.sum(jnp.sum(acc * diagonal, axis=0, keepdims=True), axis=1, keepdims=True)
    scale = 1.0 / (trace * (4.25 / (blocks * width)) + 0.5)
    scale_ref[...] = jnp.broadcast_to(scale, (1, 128))


def apply_operator(
    table_ref, vec_ref, shift_ref, scale_ref, recv_refs, edge_ref,
    gather_ref, scatter_ref, wide_ref, scratch, *, half, merged, sure,
):
    sources_ref, lhs_ref, prod_ref = scratch
    nb, width = vec_ref.shape
    blocks = wide_ref.shape[0]
    chunks = GROUP // SLOT
    levels = len(recv_refs)
    vec = vec_ref[...]
    sources_ref[0:nb, :] = halves_wide(vec)
    for level, ref in enumerate(recv_refs):
        start = nb + level * half
        sources_ref[start : start + half, :] = halves_wide(ref[0:half, :])
    start = nb + levels * half
    mine = recv_refs[merged][half : half + 8, :] if merged >= 0 else edge_ref[8:16, :]
    sources_ref[start : start + 16, :] = halves_wide(jnp.concatenate([mine, edge_ref[0:8, :]], axis=0))
    rest = sources_ref.shape[0] - start - 16
    if rest:
        sources_ref[start + 16 :, :] = jnp.zeros((rest, 2 * width), BF16)

    def stage(picked):
        picked = picked[:, :width] + picked[:, width:]
        high, low = halves(picked)
        for chunk in range(picked.shape[0] // SLOT):
            span = slice(chunk * SLOT, (chunk + 1) * SLOT)
            yield jnp.concatenate([high[span], low[span]], axis=0).astype(BF16)

    def product(lhs, block):
        wide = dot(lhs, block)
        return wide[:SLOT, :width] + wide[:SLOT, width:] + wide[SLOT:, :width]

    def rows_of(total):
        return total[:nb, :width] + total[:nb, width:] + total[nb:, :width]

    span = sure * GROUP
    picked = dot(gather_ref[0:span, :], sources_ref[...])
    for c, lhs in enumerate(stage(picked)):
        lhs_ref[c * 2 * SLOT : (c + 1) * 2 * SLOT, :] = lhs
    for pair in range(span // SLOT // 2):
        prods = []
        for c in (2 * pair, 2 * pair + 1):
            block = wide_ref[c] if c < blocks else wide_ref[table_ref[0, c - blocks]]
            prods.append(product(lhs_ref[c * 2 * SLOT : (c + 1) * 2 * SLOT, :], block))
        prod_ref[pair * 2 * SLOT : (pair + 1) * 2 * SLOT, :] = halves_wide(jnp.concatenate(prods, axis=0))
    out = rows_of(dot(scatter_ref[:, 0:span], prod_ref[...]))

    def further(group, out):
        at = pl.ds(pl.multiple_of(blocks * SLOT + group * GROUP, GROUP), GROUP)
        lhs = list(stage(dot(gather_ref[at, :], sources_ref[...])))
        prods = [product(lhs[c], wide_ref[table_ref[0, group * chunks + c]]) for c in range(chunks)]
        return out + rows_of(dot(scatter_ref[:, at], halves_wide(jnp.concatenate(prods, axis=0))))

    out = lax.fori_loop(sure - blocks * SLOT // GROUP, (table_ref[0, 127] + chunks - 1) // chunks, further, out)
    return (shift_ref[...] * vec + out) * scale_ref[...] - SHIFT * vec


def step_kernel(*refs, levels, half, merged, sure):
    table_ref, vec_ref, shift_ref, scale_ref, *rest = refs
    recv_refs, rest = rest[:levels], rest[levels:]
    edge_ref, select_ref, gather_ref, scatter_ref, wide_ref, next_ref, *rest = rest
    sends, (send_edge_ref, *scratch) = rest[:levels], rest[levels:]
    following = apply_operator(
        table_ref, vec_ref, shift_ref, scale_ref, recv_refs, edge_ref,
        gather_ref, scatter_ref, wide_ref, scratch, half=half, merged=merged, sure=sure,
    )
    next_ref[...] = following
    send_blocks(select_ref, following, sends, send_edge_ref, merged)


PAIRS = [(i, j) for i in range(ITERS + 1) for j in range(i, ITERS + 1)]


def last_kernel(*refs, levels, half, merged, sure):
    table_ref, vec_ref, shift_ref, scale_ref, *rest = refs
    recv_refs, rest = rest[:levels], rest[levels:]
    edge_ref, gather_ref, scatter_ref, wide_ref, *rest = rest
    older, (next_ref, sums_ref, *scratch) = rest[: ITERS - 1], rest[ITERS - 1 :]
    following = apply_operator(
        table_ref, vec_ref, shift_ref, scale_ref, recv_refs, edge_ref,
        gather_ref, scatter_ref, wide_ref, scratch, half=half, merged=merged, sure=sure,
    )
    next_ref[...] = following
    basis = [ref[...] for ref in older] + [vec_ref[...], following]
    sums = [jnp.sum(basis[i] * basis[j], axis=0, keepdims=True) for i, j in PAIRS]
    sums = jnp.concatenate(sums + [jnp.zeros((1, sums[0].shape[1]), F32)] * (-len(PAIRS) % 8), axis=0)
    column = jnp.sum(sums, axis=1, keepdims=True)
    at = iota((column.shape[0], 128), 0) == iota((column.shape[0], 128), 1)
    row = jnp.sum(jnp.where(at, column, 0.0), axis=0, keepdims=True)
    sums_ref[...] = jnp.broadcast_to(row, sums_ref.shape)


def finish(sums_ref, scale_ref, *refs):
    basis_refs, (solution_ref, residual_ref) = refs[: ITERS + 1], refs[ITERS + 1 :]
    row = jnp.sum(sums_ref[...], axis=0, keepdims=True)
    lane = iota(row.shape, 1)
    gram = {}
    for index, (i, j) in enumerate(PAIRS):
        entry = jnp.sum(jnp.where(lane == index, row, 0.0), axis=1, keepdims=True)
        gram[i, j] = gram[j, i] = entry
    unscale = 1.0 / scale_ref[0:1, 0:1]
    one = jnp.ones((1, 1), F32)

    def image_of(coefs):
        out = [None] * (len(coefs) + 1)
        for k, c in enumerate(coefs):
            up = c * unscale
            out[k] = SHIFT * up if out[k] is None else out[k] + SHIFT * up
            out[k + 1] = up
        return out

    def inner(a, b):
        rows = []
        for i, x in enumerate(a):
            rows.append(x * sum(gram[i, j] * y for j, y in enumerate(b)))
        return sum(rows)

    def plus(a, factor, b):
        out = list(a) + [None] * (len(b) - len(a))
        for k, y in enumerate(b):
            out[k] = factor * y if out[k] is None else out[k] + factor * y
        return out

    residual = [one]
    field = []
    image = image_of(residual)
    norm = inner(residual, residual)
    step = norm / inner(residual, image)
    direction, along = residual, image
    for k in range(ITERS):
        field = plus(field, step, direction)
        residual = plus(residual, -step, along)
        if k + 1 < ITERS:
            image = image_of(residual)
            following = inner(residual, residual)
            product = inner(residual, image)
            ratio = following / norm
            step = following / (product - ratio * following / step)
            direction = plus(residual, ratio, direction)
            along = plus(image, ratio, along)
            norm = following
    basis = [ref[...] for ref in basis_refs]
    solution_ref[...] = sum(c * v for c, v in zip(field, basis))
    residual_ref[...] = sum(c * v for c, v in zip(residual, basis))


def params(mib):
    return pltpu.CompilerParams(vmem_limit_bytes=mib * 1024 * 1024)


def vmem(count):
    return [pl.BlockSpec(memory_space=pltpu.VMEM)] * count


def shape(dims, dtype=F32):
    return jax.ShapeDtypeStruct(dims, dtype)


def per_device(
    right_side, diag_shift, dictionary, diag_ids, diag_gain, cycle_ids, cycle_weights,
    link_rows, link_ids, link_weights, *, devices,
):
    nb = diag_ids.shape[0]
    blocks, width, _ = dictionary.shape
    _, levels, half = link_rows.shape
    bits = devices.bit_length() - 1
    masks = [2 ** (bits - 1 - level) for level in range(levels)]
    merged = masks.index(1) if 1 in masks else -1
    links = levels * half
    used = 2 * nb + links + 1
    entries = -(-used // 128) * 128
    sources = -(-(nb + links + 16) // 128) * 128
    extra = -(-(used // SLOT) // (GROUP // SLOT))
    groups = blocks * SLOT // GROUP + extra

    sure = blocks * SLOT // GROUP + 1
    parity = (lax.axis_index("rows") & 1).astype(jnp.int32)[None]
    first = right_side.reshape(nb, width)
    shifts = diag_shift.reshape(nb, width)

    send_shapes = [shape((half + 8 * (level == merged), width)) for level in range(levels)]
    edge_shape = shape((8, width))
    outs = pl.pallas_call(
        functools.partial(
            prepare, nb=nb, levels=levels, half=half, merged=merged, groups=groups, sure=sure,
            entries=entries, sources=sources,
        ),
        out_shape=send_shapes
        + [
            edge_shape,
            shape((links, nb), BF16),
            shape((groups * GROUP, sources), BF16),
            shape((2 * nb, groups * GROUP), BF16),
            shape((blocks, width, 2 * width), BF16),
            shape((1, 128), jnp.int32),
            shape((1, 128)),
        ],
        in_specs=[pl.BlockSpec(memory_space=pltpu.SMEM)] + [pl.BlockSpec(memory_space=pl.ANY)] * 2 + vmem(7),
        out_specs=vmem(levels + 7),
        scratch_shapes=[
            pltpu.VMEM((blocks, width, width), F32),
            pltpu.VMEM((nb, width), F32),
            pltpu.VMEM((sure * GROUP, entries), BF16),
            pltpu.VMEM((sources, entries), BF16),
            pltpu.VMEM((2 * nb, entries), BF16),
            pltpu.SemaphoreType.DMA((5,)),
        ],
        compiler_params=params(40),
        name="prepare",
    )(
        parity, dictionary, first, diag_ids[None], diag_gain[None], cycle_ids.T, cycle_weights.T,
        *(jnp.swapaxes(array, 0, 1) for array in (link_rows, link_ids, link_weights)),
    )
    sends, (edge, select, gather, scatter, wide, table, scale) = outs[:levels], outs[levels:]

    def exchange(sends, edge):
        near = [(i, i ^ 1) for i in range(devices)]
        far = [(i, (i + 1) % devices if i % 2 else (i - 1) % devices) for i in range(devices)]
        got = [
            lax.ppermute(sends[level], "rows", [(i, i ^ masks[level]) for i in range(devices)])
            for level in range(levels)
        ]
        edges = lax.ppermute(edge, "rows", far)
        if merged < 0:
            edges = jnp.concatenate([edges, lax.ppermute(edge, "rows", near)], axis=0)
        return got, edges

    scratch = [
        pltpu.VMEM((sources, 2 * width), BF16),
        pltpu.VMEM((2 * sure * GROUP, width), BF16),
        pltpu.VMEM((sure * GROUP, 2 * width), BF16),
    ]
    smem = [pl.BlockSpec(memory_space=pltpu.SMEM)]
    basis = [first]
    for k in range(ITERS):
        got, edges = exchange(sends, edge)
        common = dict(levels=levels, half=half, merged=merged, sure=sure)
        if k + 1 < ITERS:
            following, *outs = pl.pallas_call(
                functools.partial(step_kernel, **common),
                out_shape=[shape((nb, width))] + send_shapes + [edge_shape],
                in_specs=smem + vmem(8 + levels),
                out_specs=vmem(levels + 2),
                scratch_shapes=scratch,
                compiler_params=params(24),
                name="step",
            )(table, basis[-1], shifts, scale, *got, edges, select, gather, scatter, wide)
            sends, edge = outs[:levels], outs[levels]
        else:
            following, sums = pl.pallas_call(
                functools.partial(last_kernel, **common),
                out_shape=[shape((nb, width)), shape((devices, 128))],
                in_specs=smem + vmem(7 + levels + ITERS - 1),
                out_specs=vmem(2),
                scratch_shapes=scratch,
                compiler_params=params(24),
                name="last",
            )(table, basis[-1], shifts, scale, *got, edges, gather, scatter, wide, *basis[:-1])
        basis.append(following)
    sums = lax.all_to_all(sums, "rows", 0, 0, tiled=True)
    field, residual = pl.pallas_call(
        finish,
        out_shape=[shape((nb, width))] * 2,
        in_specs=vmem(2 + len(basis)),
        out_specs=vmem(2),
        compiler_params=params(8),
        name="finish",
    )(sums, scale, *basis)
    return field.reshape(-1), residual.reshape(-1)


def solution(mesh):
    placed = (
        P("rows"), P("rows"), P(), P("rows"), P("rows"), P("rows", None), P("rows", None),
        P("rows", None, None), P("rows", None, None), P("rows", None, None),
    )
    return jax.shard_map(
        functools.partial(per_device, devices=mesh.shape["rows"]),
        mesh=mesh, in_specs=placed, out_specs=(P("rows"), P("rows")), check_vma=False,
    )
```

```python
import functools

import jax
import jax.numpy as jnp
from jax import lax
from jax.experimental import pallas as pl
from jax.experimental.pallas import tpu as pltpu
from jax.sharding import PartitionSpec as P


ITERS = 4
SLOT = 8
GROUP = 128
SHIFT = 1.5
F32 = jnp.float32
BF16 = jnp.bfloat16


def dot(a, b, dims=((1,), (0,))):
    return lax.dot_general(a, b, (dims, ((), ())), preferred_element_type=F32)


NT = ((1,), (1,))
TN = ((0,), (0,))


def halves(x):
    high = x.astype(BF16).astype(F32)
    return high, x - high


def halves_wide(x):
    high, low = halves(x)
    return jnp.concatenate([high, low], axis=1).astype(BF16)


def iota(shape, dim):
    return lax.broadcasted_iota(jnp.int32, shape, dim)


def onehot(cond):
    return jnp.where(cond, 1.0, 0.0)


def send_blocks(select_ref, block_vec, send_refs, edge_ref, merged):
    nb = block_vec.shape[0]
    edge = jnp.concatenate([block_vec[0:1], block_vec[nb - 1 :]], axis=0)
    edge = jnp.concatenate([edge, jnp.zeros((6, block_vec.shape[1]), F32)], axis=0)
    wide = halves_wide(block_vec)
    picked = dot(select_ref[...], wide)
    width = block_vec.shape[1]
    picked = picked[:, :width] + picked[:, width:]
    half = picked.shape[0] // len(send_refs)
    for level, ref in enumerate(send_refs):
        ref[0:half, :] = picked[level * half : (level + 1) * half]
        if level == merged:
            ref[half : half + 8, :] = edge
    edge_ref[...] = edge


def prepare(
    parity_ref, dict_hbm, *refs, nb, levels, half, merged, groups, sure, entries, sources,
):
    small_hbm, refs = refs[:8], refs[8:]
    sends, (edge_ref, select_ref, gather_ref, scatter_ref, wide_ref, table_ref, scale_ref) = (
        refs[:levels], refs[levels : levels + 7],
    )
    dict_vmem, here_ref, source_ref, signed_ref, *small, small_sems, sems = refs[levels + 7 :]
    vec_vmem, own_ids_ref, own_weights_ref, near_ids_ref, near_weights_ref, *link_refs = small
    link_rows_ref, link_ids_ref, link_weights_ref = link_refs
    blocks, width, _ = dict_hbm.shape
    parts = sems.shape[0]
    per = blocks // parts

    def load(part):
        span = pl.ds(part * per, per)
        return pltpu.make_async_copy(dict_hbm.at[span], dict_vmem.at[span], sems.at[part])

    load_small = [
        pltpu.make_async_copy(source, target, small_sems.at[k])
        for k, (source, target) in enumerate(zip(small_hbm, small))
    ]
    for copy in load_small[1:] + load_small[:1]:
        copy.start()
    for part in range(parts):
        load(part).start()
    for copy in load_small[1:]:
        copy.wait()

    links = levels * half
    tail = 2 * nb + links
    pad = entries - tail - 1

    def row_of(own, near, link, last):
        pieces = [own, near] + [link[level] for level in range(levels)]
        return jnp.concatenate(pieces + [last, jnp.zeros((1, pad), last.dtype)], axis=1)

    lane = iota((1, entries), 1)
    ids = row_of(own_ids_ref[...], near_ids_ref[0:1, :], link_ids_ref, near_ids_ref[1:2, nb - 1 : nb])
    ids = jnp.where(lane > tail, -1, ids)
    weights = row_of(
        own_weights_ref[...], near_weights_ref[0:1, :], link_weights_ref, near_weights_ref[1:2, nb - 1 : nb]
    )
    zeros = jnp.zeros((1, nb), jnp.int32)
    rows = row_of(zeros, zeros, link_rows_ref, zeros[:, 0:1])
    is_lower = (lane >= nb) & (lane < 2 * nb)
    is_link = (lane >= 2 * nb) & (lane < tail)
    is_tail = lane == tail
    even = parity_ref[0] == 0
    edge_base = nb + links
    before = jnp.where(even, edge_base + 9, edge_base + 1)
    after = jnp.where(even, edge_base, edge_base + 8)
    plus = jnp.where(is_link, rows, jnp.where(is_tail, nb - 1, -1))
    plus = jnp.where(lane < nb, lane, jnp.where(is_lower, lane - nb, plus))
    minus = jnp.where(is_lower & (lane > nb), lane - nb - 1, -1)
    away = jnp.where(is_link, lane - nb, jnp.where(is_tail, after, -1))
    away = jnp.where(is_lower, jnp.where(lane > nb, lane - nb - 1, before), away)

    member = onehot(iota((blocks, entries), 0) == ids)
    earlier = onehot(iota((entries, entries), 0) < iota((entries, entries), 1)).astype(BF16)
    ahead = dot(member.astype(BF16), earlier)
    rank = jnp.sum(member * ahead, axis=0, keepdims=True)
    count = jnp.sum(member, axis=1, keepdims=True)
    more = jnp.maximum(jnp.floor((count - 1.0) * (1.0 / SLOT)), 0.0)
    before_block = onehot(iota((blocks, blocks), 1) < iota((blocks, blocks), 0)).astype(BF16)
    more_wide = jnp.broadcast_to(more, (blocks, 128))
    base = dot(before_block, more_wide.astype(BF16))
    base_entry = jnp.sum(member * base[:, 0:1], axis=0, keepdims=True)
    chunk = jnp.floor(rank * (1.0 / SLOT))
    place = rank - SLOT * chunk
    idf = ids.astype(F32)
    slot = jnp.where(
        chunk == 0.0,
        idf * SLOT + place,
        (blocks + base_entry + chunk - 1.0) * SLOT + place,
    )
    slot = jnp.where(ids >= 0, slot, -1.0).astype(jnp.int32)

    chunk_lane = iota((blocks, 128), 1).astype(F32)
    owner = (chunk_lane >= base) & (chunk_lane < base + more_wide)
    block_id = iota((blocks, 128), 0).astype(F32)
    table = jnp.sum(jnp.where(owner, block_id, 0.0), axis=0, keepdims=True)
    total = jnp.sum(more_wide, axis=0, keepdims=True)
    table_ref[...] = jnp.where(iota((1, 128), 1) == 127, total, table).astype(jnp.int32)

    row_iota = iota((nb, entries), 0)
    target = onehot(row_iota == plus)
    source_iota = iota((sources, entries), 0)
    source_ref[...] = (onehot(source_iota == plus) - onehot(source_iota == away)).astype(BF16)
    signed = target - onehot(row_iota == minus)
    high, low = halves(weights)
    signed_ref[...] = jnp.concatenate([signed * high, signed * low], axis=0).astype(BF16)
    span = sure * GROUP
    here_ref[...] = onehot(iota((span, entries), 0) == slot).astype(BF16)
    gather_ref[0:span, :] = dot(here_ref[...], source_ref[...], NT).astype(BF16)
    scatter_ref[:, 0:span] = dot(signed_ref[...], here_ref[...], NT).astype(BF16)
    used_chunks = jnp.sum(more).astype(jnp.int32)
    chunks = GROUP // SLOT
    for group in range(sure, groups):

        @pl.when(used_chunks > (group - blocks * SLOT // GROUP) * chunks)
        def _(group=group):
            at = slice(group * GROUP, (group + 1) * GROUP)
            here = onehot(iota((GROUP, entries), 0) + group * GROUP == slot).astype(BF16)
            gather_ref[at, :] = dot(here, source_ref[...], NT).astype(BF16)
            scatter_ref[:, at] = dot(signed_ref[...], here, NT).astype(BF16)

    eye = onehot(iota((nb, nb), 0) == iota((nb, nb), 1)).astype(BF16)
    select_ref[...] = dot(target[:, 2 * nb : tail].astype(BF16), eye, TN).astype(BF16)
    load_small[0].wait()
    send_blocks(select_ref, vec_vmem[...], sends, edge_ref, merged)

    def split_block(k, acc):
        block = dict_vmem[k]
        block_high = block.astype(BF16)
        wide_ref[k, :, 0:width] = block_high
        wide_ref[k, :, width : 2 * width] = (block - block_high.astype(F32)).astype(BF16)
        return acc + block

    acc = jnp.zeros((width, width), F32)
    for part in range(parts):
        load(part).wait()
        acc = lax.fori_loop(part * per, (part + 1) * per, split_block, acc, unroll=4)
    diagonal = onehot(iota((width, width), 0) == iota((width, width), 1))
    trace = jnp.sum(jnp.sum(acc * diagonal, axis=0, keepdims=True), axis=1, keepdims=True)
    scale = 1.0 / (trace * (4.25 / (blocks * width)) + 0.5)
    scale_ref[...] = jnp.broadcast_to(scale, (1, 128))


def apply_operator(
    table_ref, vec_ref, shift_ref, scale_ref, recv_refs, edge_ref,
    gather_ref, scatter_ref, wide_ref, scratch, *, half, merged, sure,
):
    sources_ref, lhs_ref, prod_ref = scratch
    nb, width = vec_ref.shape
    blocks = wide_ref.shape[0]
    chunks = GROUP // SLOT
    levels = len(recv_refs)
    vec = vec_ref[...]
    sources_ref[0:nb, :] = halves_wide(vec)
    for level, ref in enumerate(recv_refs):
        start = nb + level * half
        sources_ref[start : start + half, :] = halves_wide(ref[0:half, :])
    start = nb + levels * half
    mine = recv_refs[merged][half : half + 8, :] if merged >= 0 else edge_ref[8:16, :]
    sources_ref[start : start + 16, :] = halves_wide(jnp.concatenate([mine, edge_ref[0:8, :]], axis=0))
    rest = sources_ref.shape[0] - start - 16
    if rest:
        sources_ref[start + 16 :, :] = jnp.zeros((rest, 2 * width), BF16)

    def stage(picked):
        picked = picked[:, :width] + picked[:, width:]
        high, low = halves(picked)
        for chunk in range(picked.shape[0] // SLOT):
            span = slice(chunk * SLOT, (chunk + 1) * SLOT)
            yield jnp.concatenate([high[span], low[span]], axis=0).astype(BF16)

    def product(lhs, block):
        wide = dot(lhs, block)
        return wide[:SLOT, :width] + wide[:SLOT, width:] + wide[SLOT:, :width]

    def rows_of(total):
        return total[:nb, :width] + total[:nb, width:] + total[nb:, :width]

    span = sure * GROUP
    picked = dot(gather_ref[0:span, :], sources_ref[...])
    for c, lhs in enumerate(stage(picked)):
        lhs_ref[c * 2 * SLOT : (c + 1) * 2 * SLOT, :] = lhs
    for pair in range(span // SLOT // 2):
        prods = []
        for c in (2 * pair, 2 * pair + 1):
            block = wide_ref[c] if c < blocks else wide_ref[table_ref[0, c - blocks]]
            prods.append(product(lhs_ref[c * 2 * SLOT : (c + 1) * 2 * SLOT, :], block))
        prod_ref[pair * 2 * SLOT : (pair + 1) * 2 * SLOT, :] = halves_wide(jnp.concatenate(prods, axis=0))
    out = rows_of(dot(scatter_ref[:, 0:span], prod_ref[...]))

    def further(group, out):
        at = pl.ds(pl.multiple_of(blocks * SLOT + group * GROUP, GROUP), GROUP)
        lhs = list(stage(dot(gather_ref[at, :], sources_ref[...])))
        prods = [product(lhs[c], wide_ref[table_ref[0, group * chunks + c]]) for c in range(chunks)]
        return out + rows_of(dot(scatter_ref[:, at], halves_wide(jnp.concatenate(prods, axis=0))))

    out = lax.fori_loop(sure - blocks * SLOT // GROUP, (table_ref[0, 127] + chunks - 1) // chunks, further, out)
    return (shift_ref[...] * vec + out) * scale_ref[...] - SHIFT * vec


def step_kernel(*refs, levels, half, merged, sure):
    table_ref, vec_ref, shift_ref, scale_ref, *rest = refs
    recv_refs, rest = rest[:levels], rest[levels:]
    edge_ref, select_ref, gather_ref, scatter_ref, wide_ref, next_ref, *rest = rest
    sends, (send_edge_ref, *scratch) = rest[:levels], rest[levels:]
    following = apply_operator(
        table_ref, vec_ref, shift_ref, scale_ref, recv_refs, edge_ref,
        gather_ref, scatter_ref, wide_ref, scratch, half=half, merged=merged, sure=sure,
    )
    next_ref[...] = following
    send_blocks(select_ref, following, sends, send_edge_ref, merged)


PAIRS = [(i, j) for i in range(ITERS + 1) for j in range(i, ITERS + 1)]


def last_kernel(*refs, levels, half, merged, sure):
    table_ref, vec_ref, shift_ref, scale_ref, *rest = refs
    recv_refs, rest = rest[:levels], rest[levels:]
    edge_ref, gather_ref, scatter_ref, wide_ref, *rest = rest
    older, (next_ref, sums_ref, *scratch) = rest[: ITERS - 1], rest[ITERS - 1 :]
    following = apply_operator(
        table_ref, vec_ref, shift_ref, scale_ref, recv_refs, edge_ref,
        gather_ref, scatter_ref, wide_ref, scratch, half=half, merged=merged, sure=sure,
    )
    next_ref[...] = following
    basis = [ref[...] for ref in older] + [vec_ref[...], following]
    sums = [jnp.sum(basis[i] * basis[j], axis=0, keepdims=True) for i, j in PAIRS]
    sums = jnp.concatenate(sums + [jnp.zeros((1, sums[0].shape[1]), F32)] * (-len(PAIRS) % 8), axis=0)
    column = jnp.sum(sums, axis=1, keepdims=True)
    at = iota((column.shape[0], 128), 0) == iota((column.shape[0], 128), 1)
    row = jnp.sum(jnp.where(at, column, 0.0), axis=0, keepdims=True)
    sums_ref[...] = jnp.broadcast_to(row, sums_ref.shape)


def finish(sums_ref, scale_ref, *refs):
    basis_refs, (solution_ref, residual_ref) = refs[: ITERS + 1], refs[ITERS + 1 :]
    row = jnp.sum(sums_ref[...], axis=0, keepdims=True)
    lane = iota(row.shape, 1)
    gram = {}
    for index, (i, j) in enumerate(PAIRS):
        entry = jnp.sum(jnp.where(lane == index, row, 0.0), axis=1, keepdims=True)
        gram[i, j] = gram[j, i] = entry
    unscale = 1.0 / scale_ref[0:1, 0:1]
    one = jnp.ones((1, 1), F32)

    def image_of(coefs):
        out = [None] * (len(coefs) + 1)
        for k, c in enumerate(coefs):
            up = c * unscale
            out[k] = SHIFT * up if out[k] is None else out[k] + SHIFT * up
            out[k + 1] = up
        return out

    def inner(a, b):
        rows = []
        for i, x in enumerate(a):
            rows.append(x * sum(gram[i, j] * y for j, y in enumerate(b)))
        return sum(rows)

    def plus(a, factor, b):
        out = list(a) + [None] * (len(b) - len(a))
        for k, y in enumerate(b):
            out[k] = factor * y if out[k] is None else out[k] + factor * y
        return out

    residual = [one]
    field = []
    image = image_of(residual)
    norm = inner(residual, residual)
    step = norm / inner(residual, image)
    direction, along = residual, image
    for k in range(ITERS):
        field = plus(field, step, direction)
        residual = plus(residual, -step, along)
        if k + 1 < ITERS:
            image = image_of(residual)
            following = inner(residual, residual)
            product = inner(residual, image)
            ratio = following / norm
            step = following / (product - ratio * following / step)
            direction = plus(residual, ratio, direction)
            along = plus(image, ratio, along)
            norm = following
    basis = [ref[...] for ref in basis_refs]
    solution_ref[...] = sum(c * v for c, v in zip(field, basis))
    residual_ref[...] = sum(c * v for c, v in zip(residual, basis))


def params(mib):
    return pltpu.CompilerParams(vmem_limit_bytes=mib * 1024 * 1024)


def vmem(count):
    return [pl.BlockSpec(memory_space=pltpu.VMEM)] * count


def shape(dims, dtype=F32):
    return jax.ShapeDtypeStruct(dims, dtype)


def per_device(
    right_side, diag_shift, dictionary, diag_ids, diag_gain, cycle_ids, cycle_weights,
    link_rows, link_ids, link_weights, *, devices,
):
    nb = diag_ids.shape[0]
    blocks, width, _ = dictionary.shape
    _, levels, half = link_rows.shape
    bits = devices.bit_length() - 1
    masks = [2 ** (bits - 1 - level) for level in range(levels)]
    merged = masks.index(1) if 1 in masks else -1
    links = levels * half
    used = 2 * nb + links + 1
    entries = -(-used // 128) * 128
    sources = -(-(nb + links + 16) // 128) * 128
    extra = -(-(used // SLOT) // (GROUP // SLOT))
    groups = blocks * SLOT // GROUP + extra

    sure = blocks * SLOT // GROUP + 1
    parity = (lax.axis_index("rows") & 1).astype(jnp.int32)[None]
    first = right_side.reshape(nb, width)
    shifts = diag_shift.reshape(nb, width)

    small = [first, diag_ids[None], diag_gain[None], cycle_ids.T, cycle_weights.T]
    small += [jnp.swapaxes(array, 0, 1) for array in (link_rows, link_ids, link_weights)]
    send_shapes = [shape((half + 8 * (level == merged), width)) for level in range(levels)]
    edge_shape = shape((8, width))
    outs = pl.pallas_call(
        functools.partial(
            prepare, nb=nb, levels=levels, half=half, merged=merged, groups=groups, sure=sure,
            entries=entries, sources=sources,
        ),
        out_shape=send_shapes
        + [
            edge_shape,
            shape((links, nb), BF16),
            shape((groups * GROUP, sources), BF16),
            shape((2 * nb, groups * GROUP), BF16),
            shape((blocks, width, 2 * width), BF16),
            shape((1, 128), jnp.int32),
            shape((1, 128)),
        ],
        in_specs=[pl.BlockSpec(memory_space=pltpu.SMEM)] + [pl.BlockSpec(memory_space=pltpu.HBM)] * 9,
        out_specs=vmem(levels + 7),
        scratch_shapes=[
            pltpu.VMEM((blocks, width, width), F32),
            pltpu.VMEM((sure * GROUP, entries), BF16),
            pltpu.VMEM((sources, entries), BF16),
            pltpu.VMEM((2 * nb, entries), BF16),
            *(pltpu.VMEM(array.shape, array.dtype) for array in small),
            pltpu.SemaphoreType.DMA((len(small),)),
            pltpu.SemaphoreType.DMA((4,)),
        ],
        compiler_params=params(40),
        name="prepare",
)(parity, *(pltpu.with_memory_space_constraint(array, pltpu.HBM) for array in [dictionary] + small))
    sends, (edge, select, gather, scatter, wide, table, scale) = outs[:levels], outs[levels:]

    def exchange(sends, edge):
        near = [(i, i ^ 1) for i in range(devices)]
        far = [(i, (i + 1) % devices if i % 2 else (i - 1) % devices) for i in range(devices)]
        edges = lax.ppermute(edge, "rows", far)
        if merged < 0:
            edges = jnp.concatenate([edges, lax.ppermute(edge, "rows", near)], axis=0)
        got = []
        for level in range(levels):
            pairs = [(i, i ^ masks[level]) for i in range(devices)]
            got.append(lax.ppermute(sends[level], "rows", pairs))
        return got, edges

    scratch = [
        pltpu.VMEM((sources, 2 * width), BF16),
        pltpu.VMEM((2 * sure * GROUP, width), BF16),
        pltpu.VMEM((sure * GROUP, 2 * width), BF16),
    ]
    smem = [pl.BlockSpec(memory_space=pltpu.SMEM)]
    basis = [first]
    for k in range(ITERS):
        got, edges = exchange(sends, edge)
        common = dict(levels=levels, half=half, merged=merged, sure=sure)
        if k + 1 < ITERS:
            following, *outs = pl.pallas_call(
                functools.partial(step_kernel, **common),
                out_shape=[shape((nb, width))] + send_shapes + [edge_shape],
                in_specs=smem + vmem(8 + levels),
                out_specs=vmem(levels + 2),
                scratch_shapes=scratch,
                compiler_params=params(24),
                name="step",
            )(table, basis[-1], shifts, scale, *got, edges, select, gather, scatter, wide)
            sends, edge = outs[:levels], outs[levels]
        else:
            following, sums = pl.pallas_call(
                functools.partial(last_kernel, **common),
                out_shape=[shape((nb, width)), shape((devices, 128))],
                in_specs=smem + vmem(7 + levels + ITERS - 1),
                out_specs=vmem(2),
                scratch_shapes=scratch,
                compiler_params=params(24),
                name="last",
            )(table, basis[-1], shifts, scale, *got, edges, gather, scatter, wide, *basis[:-1])
        basis.append(following)
    sums = lax.all_to_all(sums, "rows", 0, 0, tiled=True)
    field, residual = pl.pallas_call(
        finish,
        out_shape=[shape((nb, width))] * 2,
        in_specs=vmem(2 + len(basis)),
        out_specs=vmem(2),
        compiler_params=params(8),
        name="finish",
    )(sums, scale, *basis)
    return field.reshape(-1), residual.reshape(-1)


def solution(mesh):
    placed = (
        P("rows"), P("rows"), P(), P("rows"), P("rows"), P("rows", None), P("rows", None),
        P("rows", None, None), P("rows", None, None), P("rows", None, None),
    )
    return jax.shard_map(
        functools.partial(per_device, devices=mesh.shape["rows"]),
        mesh=mesh, in_specs=placed, out_specs=(P("rows"), P("rows")), check_vma=False,
    )
```

```python
import functools

import jax
import jax.numpy as jnp
from jax import lax
from jax.experimental import pallas as pl
from jax.experimental.pallas import tpu as pltpu
from jax.sharding import PartitionSpec as P


ITERS = 4
SLOT = 8
GROUP = 128
SHIFT = 1.5
F32 = jnp.float32
BF16 = jnp.bfloat16


def dot(a, b, dims=((1,), (0,))):
    return lax.dot_general(a, b, (dims, ((), ())), preferred_element_type=F32)


NT = ((1,), (1,))
TN = ((0,), (0,))


def halves(x):
    high = x.astype(BF16).astype(F32)
    return high, x - high


def halves_wide(x):
    high, low = halves(x)
    return jnp.concatenate([high, low], axis=1).astype(BF16)


def iota(shape, dim):
    return lax.broadcasted_iota(jnp.int32, shape, dim)


def onehot(cond):
    return jnp.where(cond, 1.0, 0.0)


def send_blocks(select_ref, block_vec, send_refs, edge_ref, merged):
    nb = block_vec.shape[0]
    edge = jnp.concatenate([block_vec[0:1], block_vec[nb - 1 :]], axis=0)
    edge = jnp.concatenate([edge, jnp.zeros((6, block_vec.shape[1]), F32)], axis=0)
    wide = halves_wide(block_vec)
    picked = dot(select_ref[...], wide)
    width = block_vec.shape[1]
    picked = picked[:, :width] + picked[:, width:]
    half = picked.shape[0] // len(send_refs)
    for level, ref in enumerate(send_refs):
        ref[0:half, :] = picked[level * half : (level + 1) * half]
        if level == merged:
            ref[half : half + 8, :] = edge
    edge_ref[...] = edge


def prepare(
    parity_ref, dict_hbm, *refs, nb, levels, half, merged, groups, sure, entries, sources,
):
    small_hbm, refs = refs[:8], refs[8:]
    sends, (edge_ref, select_ref, gather_ref, scatter_ref, dict_vmem, table_ref) = (
        refs[:levels], refs[levels : levels + 6],
    )
    facts_ref, *small, small_sems, sems = refs[levels + 6 :]
    vec_vmem, own_ids_ref, own_weights_ref, near_ids_ref, near_weights_ref, *link_refs = small
    link_rows_ref, link_ids_ref, link_weights_ref = link_refs
    blocks, _, _ = dict_hbm.shape
    parts = sems.shape[0]
    per = blocks // parts

    def load(part):
        span = pl.ds(part * per, per)
        return pltpu.make_async_copy(dict_hbm.at[span], dict_vmem.at[span], sems.at[part])

    load_small = [
        pltpu.make_async_copy(source, target, small_sems.at[k])
        for k, (source, target) in enumerate(zip(small_hbm, small))
    ]
    for copy in load_small[1:] + load_small[:1]:
        copy.start()
    for part in range(parts):
        load(part).start()
    for copy in load_small[1:]:
        copy.wait()

    links = levels * half
    tail = 2 * nb + links
    pad = entries - tail - 1

    def row_of(own, near, link, last):
        pieces = [own, near] + [link[level] for level in range(levels)]
        return jnp.concatenate(pieces + [last, jnp.zeros((1, pad), last.dtype)], axis=1)

    lane = iota((1, entries), 1)
    ids = row_of(own_ids_ref[...], near_ids_ref[0:1, :], link_ids_ref, near_ids_ref[1:2, nb - 1 : nb])
    ids = jnp.where(lane > tail, -1, ids)
    weights = row_of(
        own_weights_ref[...], near_weights_ref[0:1, :], link_weights_ref, near_weights_ref[1:2, nb - 1 : nb]
    )
    zeros = jnp.zeros((1, nb), jnp.int32)
    rows = row_of(zeros, zeros, link_rows_ref, zeros[:, 0:1])
    is_lower = (lane >= nb) & (lane < 2 * nb)
    is_link = (lane >= 2 * nb) & (lane < tail)
    is_tail = lane == tail
    even = parity_ref[0] == 0
    edge_base = nb + links
    before = jnp.where(even, edge_base + 9, edge_base + 1)
    after = jnp.where(even, edge_base, edge_base + 8)
    plus = jnp.where(is_link, rows, jnp.where(is_tail, nb - 1, -1))
    plus = jnp.where(lane < nb, lane, jnp.where(is_lower, lane - nb, plus))
    minus = jnp.where(is_lower & (lane > nb), lane - nb - 1, -1)
    away = jnp.where(is_link, lane - nb, jnp.where(is_tail, after, -1))
    away = jnp.where(is_lower, jnp.where(lane > nb, lane - nb - 1, before), away)

    eye = onehot(iota((nb, nb), 0) == iota((nb, nb), 1)).astype(BF16)
    linked = onehot(iota((nb, links), 0) == plus[:, 2 * nb : tail]).astype(BF16)
    select_ref[...] = dot(linked, eye, TN).astype(BF16)

    member = onehot(iota((blocks, entries), 0) == ids)
    earlier = onehot(iota((128, 128), 0) < iota((128, 128), 1)).astype(BF16)
    ahead = []
    so_far = jnp.zeros((blocks, 1), F32)
    for start in range(0, entries, 128):
        part = member[:, start : start + 128]
        ahead.append(dot(part.astype(BF16), earlier) + so_far)
        so_far = so_far + jnp.sum(part, axis=1, keepdims=True)
    rank = jnp.sum(member * jnp.concatenate(ahead, axis=1), axis=0, keepdims=True)
    count = so_far
    more = jnp.maximum(jnp.floor((count - 1.0) * (1.0 / SLOT)), 0.0)
    before_block = onehot(iota((blocks, blocks), 1) < iota((blocks, blocks), 0)).astype(BF16)
    more_wide = jnp.broadcast_to(more, (blocks, 128))
    base = dot(before_block, more_wide.astype(BF16))
    base_entry = jnp.sum(member * base[:, 0:1], axis=0, keepdims=True)
    chunk = jnp.floor(rank * (1.0 / SLOT))
    place = rank - SLOT * chunk
    idf = ids.astype(F32)
    slot = jnp.where(
        chunk == 0.0,
        idf * SLOT + place,
        (blocks + base_entry + chunk - 1.0) * SLOT + place,
    )
    slot = jnp.where(ids >= 0, slot, -1.0).astype(jnp.int32)

    chunk_lane = iota((blocks, 128), 1).astype(F32)
    owner = (chunk_lane >= base) & (chunk_lane < base + more_wide)
    block_id = iota((blocks, 128), 0).astype(F32)
    table = jnp.sum(jnp.where(owner, block_id, 0.0), axis=0, keepdims=True)
    total = jnp.sum(more_wide, axis=0, keepdims=True)
    table_ref[...] = jnp.where(iota((1, 128), 1) == 127, total, table).astype(jnp.int32)

    high, low = halves(weights)
    absent = away < 0
    facts = [
        plus.astype(F32), jnp.where(absent, 256, away - 256).astype(F32), minus.astype(F32), high, low,
    ]
    facts = jnp.concatenate(facts + [jnp.zeros((128 - len(facts), entries), F32)], axis=0)
    facts_ref[...] = facts.astype(BF16)

    def fill(start, count):
        here = onehot(iota((count, entries), 0) + start == slot).astype(BF16)
        known = dot(here, facts_ref[...], NT)
        source = iota((count, sources), 1).astype(F32)
        picked = jnp.where(source == known[:, 0:1], 1.0, jnp.where(source - 256.0 == known[:, 1:2], -1.0, 0.0))
        gather_ref[start : start + count, :] = picked.astype(BF16)
        for at in range(0, count, 128):
            across = known[at : at + 128].T
            row = iota((nb, 128), 0).astype(F32)
            up, down = row == across[0:1], row == across[2:3]
            span = slice(start + at, start + at + 128)
            for half_index in range(2):
                weight = across[3 + half_index : 4 + half_index]
                signed = jnp.where(up, weight, jnp.where(down, -weight, 0.0))
                scatter_ref[half_index * nb : (half_index + 1) * nb, span] = signed.astype(BF16)

    fill(0, sure * GROUP)
    used_chunks = jnp.sum(more).astype(jnp.int32)
    chunks = GROUP // SLOT
    for group in range(sure, groups):

        @pl.when(used_chunks > (group - blocks * SLOT // GROUP) * chunks)
        def _(group=group):
            fill(group * GROUP, GROUP)

    load_small[0].wait()
    send_blocks(select_ref, vec_vmem[...], sends, edge_ref, merged)
    for part in range(parts):
        load(part).wait()


def apply_operator(
    table_ref, vec_ref, shift_ref, scale_ref, recv_refs, edge_ref,
    gather_ref, scatter_ref, wide_ref, scratch, *, half, merged, sure, dict_ref=None,
):
    sources_ref, lhs_ref, prod_ref, table_smem, table_sem = scratch
    copy_table = pltpu.make_async_copy(table_ref, table_smem, table_sem)
    copy_table.start()
    nb, width = vec_ref.shape
    blocks = wide_ref.shape[0]
    chunks = GROUP // SLOT
    levels = len(recv_refs)
    vec = vec_ref[...]
    sources_ref[0:nb, :] = halves_wide(vec)
    for level, ref in enumerate(recv_refs):
        start = nb + level * half
        sources_ref[start : start + half, :] = halves_wide(ref[0:half, :])
    start = nb + levels * half
    mine = recv_refs[merged][half : half + 8, :] if merged >= 0 else edge_ref[8:16, :]
    sources_ref[start : start + 16, :] = halves_wide(jnp.concatenate([mine, edge_ref[0:8, :]], axis=0))
    rest = sources_ref.shape[0] - start - 16
    if rest:
        sources_ref[start + 16 :, :] = jnp.zeros((rest, 2 * width), BF16)

    def stage(picked):
        picked = picked[:, :width] + picked[:, width:]
        high, low = halves(picked)
        for chunk in range(picked.shape[0] // SLOT):
            span = slice(chunk * SLOT, (chunk + 1) * SLOT)
            yield jnp.concatenate([high[span], low[span]], axis=0).astype(BF16)

    def product(lhs, block):
        wide = dot(lhs, block)
        return wide[:SLOT, :width] + wide[:SLOT, width:] + wide[SLOT:, :width]

    def rows_of(total):
        return total[:nb, :width] + total[:nb, width:] + total[nb:, :width]

    span = sure * GROUP
    picked = dot(gather_ref[0:span, :], sources_ref[...])
    for c, lhs in enumerate(stage(picked)):
        lhs_ref[c * 2 * SLOT : (c + 1) * 2 * SLOT, :] = lhs
    total = jnp.zeros((width, width), F32)
    for pair in range(span // SLOT // 2):
        prods = []
        for c in (2 * pair, 2 * pair + 1):
            if c == blocks:
                copy_table.wait()
            if c >= blocks:
                block = wide_ref[table_smem[0, c - blocks]]
            elif dict_ref is None:
                block = wide_ref[c]
            else:
                block = dict_ref[c]
                total = total + block
                block = halves_wide(block)
                wide_ref[c] = block
            prods.append(product(lhs_ref[c * 2 * SLOT : (c + 1) * 2 * SLOT, :], block))
        prod_ref[pair * 2 * SLOT : (pair + 1) * 2 * SLOT, :] = halves_wide(jnp.concatenate(prods, axis=0))
    out = rows_of(dot(scatter_ref[:, 0:span], prod_ref[...]))

    def further(group, out):
        at = pl.ds(pl.multiple_of(blocks * SLOT + group * GROUP, GROUP), GROUP)
        lhs = list(stage(dot(gather_ref[at, :], sources_ref[...])))
        prods = [product(lhs[c], wide_ref[table_smem[0, group * chunks + c]]) for c in range(chunks)]
        return out + rows_of(dot(scatter_ref[:, at], halves_wide(jnp.concatenate(prods, axis=0))))

    out = lax.fori_loop(sure - blocks * SLOT // GROUP, (table_smem[0, 127] + chunks - 1) // chunks, further, out)
    if dict_ref is not None:
        diagonal = onehot(iota((width, width), 0) == iota((width, width), 1))
        trace = jnp.sum(jnp.sum(total * diagonal, axis=0, keepdims=True), axis=1, keepdims=True)
        scale = 1.0 / (trace * (4.25 / (blocks * width)) + 0.5)
        scale_ref[...] = jnp.broadcast_to(scale, (1, 128))
    return (shift_ref[...] * vec + out) * scale_ref[...] - SHIFT * vec


def first_kernel(*refs, levels, half, merged, sure):
    table_ref, vec_ref, shift_ref, *rest = refs
    recv_refs, rest = rest[:levels], rest[levels:]
    edge_ref, select_ref, gather_ref, scatter_ref, dict_ref, next_ref, *rest = rest
    sends, (send_edge_ref, wide_ref, scale_ref, *scratch) = rest[:levels], rest[levels:]
    following = apply_operator(
        table_ref, vec_ref, shift_ref, scale_ref, recv_refs, edge_ref,
        gather_ref, scatter_ref, wide_ref, scratch, half=half, merged=merged, sure=sure, dict_ref=dict_ref,
    )
    next_ref[...] = following
    send_blocks(select_ref, following, sends, send_edge_ref, merged)


def step_kernel(*refs, levels, half, merged, sure):
    table_ref, vec_ref, shift_ref, scale_ref, *rest = refs
    recv_refs, rest = rest[:levels], rest[levels:]
    edge_ref, select_ref, gather_ref, scatter_ref, wide_ref, next_ref, *rest = rest
    sends, (send_edge_ref, *scratch) = rest[:levels], rest[levels:]
    following = apply_operator(
        table_ref, vec_ref, shift_ref, scale_ref, recv_refs, edge_ref,
        gather_ref, scatter_ref, wide_ref, scratch, half=half, merged=merged, sure=sure,
    )
    next_ref[...] = following
    send_blocks(select_ref, following, sends, send_edge_ref, merged)


PAIRS = [(i, j) for i in range(ITERS + 1) for j in range(i, ITERS + 1)]


def last_kernel(*refs, levels, half, merged, sure):
    table_ref, vec_ref, shift_ref, scale_ref, *rest = refs
    recv_refs, rest = rest[:levels], rest[levels:]
    edge_ref, gather_ref, scatter_ref, wide_ref, *rest = rest
    older, (next_ref, sums_ref, *scratch) = rest[: ITERS - 1], rest[ITERS - 1 :]
    following = apply_operator(
        table_ref, vec_ref, shift_ref, scale_ref, recv_refs, edge_ref,
        gather_ref, scatter_ref, wide_ref, scratch, half=half, merged=merged, sure=sure,
    )
    next_ref[...] = following
    basis = [ref[...] for ref in older] + [vec_ref[...], following]
    sums = [jnp.sum(basis[i] * basis[j], axis=0, keepdims=True) for i, j in PAIRS]
    sums = jnp.concatenate(sums + [jnp.zeros((1, sums[0].shape[1]), F32)] * (-len(PAIRS) % 8), axis=0)
    column = jnp.sum(sums, axis=1, keepdims=True)
    at = iota((column.shape[0], 128), 0) == iota((column.shape[0], 128), 1)
    row = jnp.sum(jnp.where(at, column, 0.0), axis=0, keepdims=True)
    sums_ref[...] = jnp.broadcast_to(row, sums_ref.shape)


def finish(sums_ref, scale_ref, *refs):
    basis_refs, (solution_ref, residual_ref) = refs[: ITERS + 1], refs[ITERS + 1 :]
    row = jnp.sum(sums_ref[...], axis=0, keepdims=True)
    lane = iota(row.shape, 1)
    gram = {}
    for index, (i, j) in enumerate(PAIRS):
        entry = jnp.sum(jnp.where(lane == index, row, 0.0), axis=1, keepdims=True)
        gram[i, j] = gram[j, i] = entry
    unscale = 1.0 / scale_ref[0:1, 0:1]
    one = jnp.ones((1, 1), F32)

    def image_of(coefs):
        out = [None] * (len(coefs) + 1)
        for k, c in enumerate(coefs):
            up = c * unscale
            out[k] = SHIFT * up if out[k] is None else out[k] + SHIFT * up
            out[k + 1] = up
        return out

    def inner(a, b):
        rows = []
        for i, x in enumerate(a):
            rows.append(x * sum(gram[i, j] * y for j, y in enumerate(b)))
        return sum(rows)

    def plus(a, factor, b):
        out = list(a) + [None] * (len(b) - len(a))
        for k, y in enumerate(b):
            out[k] = factor * y if out[k] is None else out[k] + factor * y
        return out

    residual = [one]
    field = []
    image = image_of(residual)
    norm = inner(residual, residual)
    step = norm / inner(residual, image)
    direction, along = residual, image
    for k in range(ITERS):
        field = plus(field, step, direction)
        residual = plus(residual, -step, along)
        if k + 1 < ITERS:
            image = image_of(residual)
            following = inner(residual, residual)
            product = inner(residual, image)
            ratio = following / norm
            step = following / (product - ratio * following / step)
            direction = plus(residual, ratio, direction)
            along = plus(image, ratio, along)
            norm = following
    basis = [ref[...] for ref in basis_refs]
    solution_ref[...] = sum(c * v for c, v in zip(field, basis))
    residual_ref[...] = sum(c * v for c, v in zip(residual, basis))


def params(mib):
    return pltpu.CompilerParams(vmem_limit_bytes=mib * 1024 * 1024)


def vmem(count):
    return [pl.BlockSpec(memory_space=pltpu.VMEM)] * count


def shape(dims, dtype=F32):
    return jax.ShapeDtypeStruct(dims, dtype)


def per_device(
    right_side, diag_shift, dictionary, diag_ids, diag_gain, cycle_ids, cycle_weights,
    link_rows, link_ids, link_weights, *, devices,
):
    nb = diag_ids.shape[0]
    blocks, width, _ = dictionary.shape
    _, levels, half = link_rows.shape
    bits = devices.bit_length() - 1
    masks = [2 ** (bits - 1 - level) for level in range(levels)]
    merged = masks.index(1) if 1 in masks else -1
    links = levels * half
    used = 2 * nb + links + 1
    entries = -(-used // 128) * 128
    sources = -(-(nb + links + 16) // 128) * 128
    assert sources <= 512 and nb <= 256
    extra = -(-(used // SLOT) // (GROUP // SLOT))
    groups = blocks * SLOT // GROUP + extra

    sure = blocks * SLOT // GROUP + 1
    parity = (lax.axis_index("rows") & 1).astype(jnp.int32)[None]
    first = right_side.reshape(nb, width)
    shifts = diag_shift.reshape(nb, width)

    small = [first, diag_ids[None], diag_gain[None], cycle_ids.T, cycle_weights.T]
    small += [jnp.swapaxes(array, 0, 1) for array in (link_rows, link_ids, link_weights)]
    send_shapes = [shape((half + 8 * (level == merged), width)) for level in range(levels)]
    edge_shape = shape((8, width))
    outs = pl.pallas_call(
        functools.partial(
            prepare, nb=nb, levels=levels, half=half, merged=merged, groups=groups, sure=sure,
            entries=entries, sources=sources,
        ),
        out_shape=send_shapes
        + [
            edge_shape,
            shape((links, nb), BF16),
            shape((groups * GROUP, sources), BF16),
            shape((2 * nb, groups * GROUP), BF16),
            shape((blocks, width, width)),
            shape((1, 128), jnp.int32),
        ],
        in_specs=[pl.BlockSpec(memory_space=pltpu.SMEM)] + [pl.BlockSpec(memory_space=pltpu.HBM)] * 9,
        out_specs=vmem(levels + 6),
        scratch_shapes=[
            pltpu.VMEM((128, entries), BF16),
            *(pltpu.VMEM(array.shape, array.dtype) for array in small),
            pltpu.SemaphoreType.DMA((len(small),)),
            pltpu.SemaphoreType.DMA((4,)),
        ],
        compiler_params=params(24),
        name="prepare",
)(parity, *(pltpu.with_memory_space_constraint(array, pltpu.HBM) for array in [dictionary] + small))
    sends, (edge, select, gather, scatter, blocks_vmem, table) = outs[:levels], outs[levels:]

    def exchange(sends, edge):
        near = [(i, i ^ 1) for i in range(devices)]
        far = [(i, (i + 1) % devices if i % 2 else (i - 1) % devices) for i in range(devices)]
        edges = lax.ppermute(edge, "rows", far)
        if merged < 0:
            edges = jnp.concatenate([edges, lax.ppermute(edge, "rows", near)], axis=0)
        got = []
        for level in range(levels):
            pairs = [(i, i ^ masks[level]) for i in range(devices)]
            got.append(lax.ppermute(sends[level], "rows", pairs))
        return got, edges

    scratch = [
        pltpu.VMEM((sources, 2 * width), BF16),
        pltpu.VMEM((2 * sure * GROUP, width), BF16),
        pltpu.VMEM((sure * GROUP, 2 * width), BF16),
        pltpu.SMEM((1, 128), jnp.int32),
        pltpu.SemaphoreType.DMA,
    ]
    basis = [first]
    for k in range(ITERS):
        got, edges = exchange(sends, edge)
        common = dict(levels=levels, half=half, merged=merged, sure=sure)
        if k == 0:
            following, *outs = pl.pallas_call(
                functools.partial(first_kernel, **common),
                out_shape=[shape((nb, width))] + send_shapes
                + [edge_shape, shape((blocks, width, 2 * width), BF16), shape((1, 128))],
                in_specs=vmem(8 + levels),
                out_specs=vmem(levels + 4),
                scratch_shapes=scratch,
                compiler_params=params(24),
                name="first",
            )(table, first, shifts, *got, edges, select, gather, scatter, blocks_vmem)
            sends, (edge, wide, scale) = outs[:levels], outs[levels:]
        elif k + 1 < ITERS:
            following, *outs = pl.pallas_call(
                functools.partial(step_kernel, **common),
                out_shape=[shape((nb, width))] + send_shapes + [edge_shape],
                in_specs=vmem(9 + levels),
                out_specs=vmem(levels + 2),
                scratch_shapes=scratch,
                compiler_params=params(24),
                name="step",
            )(table, basis[-1], shifts, scale, *got, edges, select, gather, scatter, wide)
            sends, edge = outs[:levels], outs[levels]
        else:
            following, sums = pl.pallas_call(
                functools.partial(last_kernel, **common),
                out_shape=[shape((nb, width)), shape((devices, 128))],
                in_specs=vmem(8 + levels + ITERS - 1),
                out_specs=vmem(2),
                scratch_shapes=scratch,
                compiler_params=params(24),
                name="last",
            )(table, basis[-1], shifts, scale, *got, edges, gather, scatter, wide, *basis[:-1])
        basis.append(following)
    sums = lax.all_to_all(sums, "rows", 0, 0, tiled=True)
    field, residual = pl.pallas_call(
        finish,
        out_shape=[shape((nb, width))] * 2,
        in_specs=vmem(2 + len(basis)),
        out_specs=vmem(2),
        compiler_params=params(8),
        name="finish",
    )(sums, scale, *basis)
    return field.reshape(-1), residual.reshape(-1)


def solution(mesh):
    placed = (
        P("rows"), P("rows"), P(), P("rows"), P("rows"), P("rows", None), P("rows", None),
        P("rows", None, None), P("rows", None, None), P("rows", None, None),
    )
    return jax.shard_map(
        functools.partial(per_device, devices=mesh.shape["rows"]),
        mesh=mesh, in_specs=placed, out_specs=(P("rows"), P("rows")), check_vma=False,
    )
```

```python
import functools

import jax
import jax.numpy as jnp
from jax import lax
from jax.experimental import pallas as pl
from jax.experimental.pallas import tpu as pltpu
from jax.sharding import PartitionSpec as P


ITERS = 4
SLOT = 8
GROUP = 128
PARTS = 3
SHIFT = 1.5
F32 = jnp.float32
BF16 = jnp.bfloat16


def dot(a, b, dims=((1,), (0,))):
    return lax.dot_general(a, b, (dims, ((), ())), preferred_element_type=F32)


NT = ((1,), (1,))
TN = ((0,), (0,))


def halves(x):
    high = x.astype(BF16).astype(F32)
    return high, x - high


def halves_wide(x):
    high, low = halves(x)
    return jnp.concatenate([high, low], axis=1).astype(BF16)


def iota(shape, dim):
    return lax.broadcasted_iota(jnp.int32, shape, dim)


def onehot(cond):
    return jnp.where(cond, 1.0, 0.0)


def send_blocks(select_ref, block_vec, send_refs, edge_ref, merged):
    nb = block_vec.shape[0]
    edge = jnp.concatenate([block_vec[0:1], block_vec[nb - 1 :]], axis=0)
    edge = jnp.concatenate([edge, jnp.zeros((6, block_vec.shape[1]), F32)], axis=0)
    wide = halves_wide(block_vec)
    picked = dot(select_ref[...], wide)
    width = block_vec.shape[1]
    picked = picked[:, :width] + picked[:, width:]
    half = picked.shape[0] // len(send_refs)
    for level, ref in enumerate(send_refs):
        ref[0:half, :] = picked[level * half : (level + 1) * half]
        if level == merged:
            ref[half : half + 8, :] = edge
    edge_ref[...] = edge


def prepare(
    parity_ref, dict_hbm, *refs, nb, levels, half, merged, groups, sure, entries, sources,
):
    small_hbm, refs = refs[:8], refs[8:]
    sends, (edge_ref, select_ref, gather_ref, scatter_ref, dict_vmem, table_ref) = (
        refs[:levels], refs[levels : levels + 6],
    )
    facts_ref, *small, small_sems, sems = refs[levels + 6 :]
    vec_vmem, own_ids_ref, own_weights_ref, near_ids_ref, near_weights_ref, *link_refs = small
    link_rows_ref, link_ids_ref, link_weights_ref = link_refs
    blocks, _, _ = dict_hbm.shape
    parts = sems.shape[0]
    per = blocks // parts

    def load(part):
        span = pl.ds(part * per, per)
        return pltpu.make_async_copy(dict_hbm.at[span], dict_vmem.at[span], sems.at[part])

    load_small = [
        pltpu.make_async_copy(source, target, small_sems.at[k])
        for k, (source, target) in enumerate(zip(small_hbm, small))
    ]
    for copy in load_small[1:] + load_small[:1]:
        copy.start()
    for part in range(parts):
        load(part).start()
    for copy in load_small[1:]:
        copy.wait()

    links = levels * half
    tail = 2 * nb + links
    pad = entries - tail - 1

    def row_of(own, near, link, last):
        pieces = [own, near] + [link[level] for level in range(levels)]
        return jnp.concatenate(pieces + [last, jnp.zeros((1, pad), last.dtype)], axis=1)

    lane = iota((1, entries), 1)
    ids = row_of(own_ids_ref[...], near_ids_ref[0:1, :], link_ids_ref, near_ids_ref[1:2, nb - 1 : nb])
    ids = jnp.where(lane > tail, -1, ids)
    weights = row_of(
        own_weights_ref[...], near_weights_ref[0:1, :], link_weights_ref, near_weights_ref[1:2, nb - 1 : nb]
    )
    zeros = jnp.zeros((1, nb), jnp.int32)
    rows = row_of(zeros, zeros, link_rows_ref, zeros[:, 0:1])
    is_lower = (lane >= nb) & (lane < 2 * nb)
    is_link = (lane >= 2 * nb) & (lane < tail)
    is_tail = lane == tail
    even = parity_ref[0] == 0
    edge_base = nb + links
    before = jnp.where(even, edge_base + 9, edge_base + 1)
    after = jnp.where(even, edge_base, edge_base + 8)
    plus = jnp.where(is_link, rows, jnp.where(is_tail, nb - 1, -1))
    plus = jnp.where(lane < nb, lane, jnp.where(is_lower, lane - nb, plus))
    minus = jnp.where(is_lower & (lane > nb), lane - nb - 1, -1)
    away = jnp.where(is_link, lane - nb, jnp.where(is_tail, after, -1))
    away = jnp.where(is_lower, jnp.where(lane > nb, lane - nb - 1, before), away)

    eye = onehot(iota((nb, nb), 0) == iota((nb, nb), 1)).astype(BF16)
    linked = onehot(iota((nb, links), 0) == plus[:, 2 * nb : tail]).astype(BF16)
    select_ref[...] = dot(linked, eye, TN).astype(BF16)

    member = onehot(iota((blocks, entries), 0) == ids)
    earlier = onehot(iota((128, 128), 0) < iota((128, 128), 1)).astype(BF16)
    ahead = []
    so_far = jnp.zeros((blocks, 1), F32)
    for start in range(0, entries, 128):
        part = member[:, start : start + 128]
        ahead.append(dot(part.astype(BF16), earlier) + so_far)
        so_far = so_far + jnp.sum(part, axis=1, keepdims=True)
    rank = jnp.sum(member * jnp.concatenate(ahead, axis=1), axis=0, keepdims=True)
    count = so_far
    more = jnp.maximum(jnp.floor((count - 1.0) * (1.0 / SLOT)), 0.0)
    before_block = onehot(iota((blocks, blocks), 1) < iota((blocks, blocks), 0)).astype(BF16)
    more_wide = jnp.broadcast_to(more, (blocks, 128))
    base = dot(before_block, more_wide.astype(BF16))
    base_entry = jnp.sum(member * base[:, 0:1], axis=0, keepdims=True)
    chunk = jnp.floor(rank * (1.0 / SLOT))
    place = rank - SLOT * chunk
    idf = ids.astype(F32)
    slot = jnp.where(
        chunk == 0.0,
        idf * SLOT + place,
        (blocks + base_entry + chunk - 1.0) * SLOT + place,
    )
    slot = jnp.where(ids >= 0, slot, -1.0).astype(jnp.int32)

    chunk_lane = iota((blocks, 128), 1).astype(F32)
    owner = (chunk_lane >= base) & (chunk_lane < base + more_wide)
    block_id = iota((blocks, 128), 0).astype(F32)
    table = jnp.sum(jnp.where(owner, block_id, 0.0), axis=0, keepdims=True)
    total = jnp.sum(more_wide, axis=0, keepdims=True)
    table_ref[...] = jnp.where(iota((1, 128), 1) == 127, total, table).astype(jnp.int32)

    high, low = halves(weights)
    absent = away < 0
    facts = [
        plus.astype(F32), jnp.where(absent, 256, away - 256).astype(F32), minus.astype(F32), high, low,
    ]
    facts = jnp.concatenate(facts + [jnp.zeros((128 - len(facts), entries), F32)], axis=0)
    facts_ref[...] = facts.astype(BF16)

    def fill(start, count):
        here = onehot(iota((count, entries), 0) + start == slot).astype(BF16)
        known = dot(here, facts_ref[...], NT)
        source = iota((count, sources), 1).astype(F32)
        picked = jnp.where(source == known[:, 0:1], 1.0, jnp.where(source - 256.0 == known[:, 1:2], -1.0, 0.0))
        gather_ref[start : start + count, :] = picked.astype(BF16)
        for at in range(0, count, 128):
            across = known[at : at + 128].T
            row = iota((nb, 128), 0).astype(F32)
            up, down = row == across[0:1], row == across[2:3]
            span = slice(start + at, start + at + 128)
            for half_index in range(2):
                weight = across[3 + half_index : 4 + half_index]
                signed = jnp.where(up, weight, jnp.where(down, -weight, 0.0))
                scatter_ref[half_index * nb : (half_index + 1) * nb, span] = signed.astype(BF16)

    fill(0, sure * GROUP)
    used_chunks = jnp.sum(more).astype(jnp.int32)
    chunks = GROUP // SLOT
    for group in range(sure, groups):

        @pl.when(used_chunks > (group - blocks * SLOT // GROUP) * chunks)
        def _(group=group):
            fill(group * GROUP, GROUP)

    load_small[0].wait()
    send_blocks(select_ref, vec_vmem[...], sends, edge_ref, merged)
    for part in range(parts):
        load(part).wait()


def apply_operator(
    table_ref, vec_ref, shift_ref, scale_ref, recv_refs, edge_ref,
    gather_ref, scatter_ref, wide_ref, scratch, *, half, merged, sure, dict_ref=None,
):
    sources_ref, lhs_ref, prod_ref, table_smem, table_sem = scratch
    copy_table = pltpu.make_async_copy(table_ref, table_smem, table_sem)
    copy_table.start()
    nb, width = vec_ref.shape
    blocks = wide_ref.shape[0]
    chunks = GROUP // SLOT
    levels = len(recv_refs)
    vec = vec_ref[...]
    sources_ref[0:nb, :] = halves_wide(vec)
    for level, ref in enumerate(recv_refs):
        start = nb + level * half
        sources_ref[start : start + half, :] = halves_wide(ref[0:half, :])
    start = nb + levels * half
    mine = recv_refs[merged][half : half + 8, :] if merged >= 0 else edge_ref[8:16, :]
    sources_ref[start : start + 16, :] = halves_wide(jnp.concatenate([mine, edge_ref[0:8, :]], axis=0))
    rest = sources_ref.shape[0] - start - 16
    if rest:
        sources_ref[start + 16 :, :] = jnp.zeros((rest, 2 * width), BF16)

    def stage(picked):
        picked = picked[:, :width] + picked[:, width:]
        high, low = halves(picked)
        for chunk in range(picked.shape[0] // SLOT):
            span = slice(chunk * SLOT, (chunk + 1) * SLOT)
            yield jnp.concatenate([high[span], low[span]], axis=0).astype(BF16)

    def product(lhs, block):
        wide = dot(lhs, block)
        return wide[:SLOT, :width] + wide[:SLOT, width:] + wide[SLOT:, :width]

    def rows_of(total):
        return total[:nb, :width] + total[:nb, width:] + total[nb:, :width]

    parts = PARTS if sure % PARTS == 0 else 1
    part_span = sure // parts * GROUP

    def gather_part(part):
        at = part * part_span
        picked = dot(gather_ref[at : at + part_span, :], sources_ref[...])
        for c, lhs in enumerate(stage(picked)):
            lhs_ref[2 * at + c * 2 * SLOT : 2 * at + (c + 1) * 2 * SLOT, :] = lhs

    total = jnp.zeros((width, width), F32)
    out = jnp.zeros((nb, width), F32)
    gather_part(0)
    for part in range(parts):
        if part + 1 < parts:
            gather_part(part + 1)
        for pair in range(part * part_span // SLOT // 2, (part + 1) * part_span // SLOT // 2):
            prods = []
            for c in (2 * pair, 2 * pair + 1):
                if c == blocks:
                    copy_table.wait()
                if c >= blocks:
                    block = wide_ref[table_smem[0, c - blocks]]
                elif dict_ref is None:
                    block = wide_ref[c]
                else:
                    block = dict_ref[c]
                    total = total + block
                    block = halves_wide(block)
                    wide_ref[c] = block
                prods.append(product(lhs_ref[c * 2 * SLOT : (c + 1) * 2 * SLOT, :], block))
            prod_ref[pair * 2 * SLOT : (pair + 1) * 2 * SLOT, :] = halves_wide(jnp.concatenate(prods, axis=0))
        span = slice(part * part_span, (part + 1) * part_span)
        out = out + rows_of(dot(scatter_ref[:, span], prod_ref[span, :]))

    def further(group, out):
        at = pl.ds(pl.multiple_of(blocks * SLOT + group * GROUP, GROUP), GROUP)
        lhs = list(stage(dot(gather_ref[at, :], sources_ref[...])))
        prods = [product(lhs[c], wide_ref[table_smem[0, group * chunks + c]]) for c in range(chunks)]
        return out + rows_of(dot(scatter_ref[:, at], halves_wide(jnp.concatenate(prods, axis=0))))

    out = lax.fori_loop(sure - blocks * SLOT // GROUP, (table_smem[0, 127] + chunks - 1) // chunks, further, out)
    if dict_ref is not None:
        diagonal = onehot(iota((width, width), 0) == iota((width, width), 1))
        trace = jnp.sum(jnp.sum(total * diagonal, axis=0, keepdims=True), axis=1, keepdims=True)
        scale = 1.0 / (trace * (4.25 / (blocks * width)) + 0.5)
        scale_ref[...] = jnp.broadcast_to(scale, (1, 128))
    return (shift_ref[...] * vec + out) * scale_ref[...] - SHIFT * vec


def first_kernel(*refs, levels, half, merged, sure):
    table_ref, vec_ref, shift_ref, *rest = refs
    recv_refs, rest = rest[:levels], rest[levels:]
    edge_ref, select_ref, gather_ref, scatter_ref, dict_ref, next_ref, *rest = rest
    sends, (send_edge_ref, wide_ref, scale_ref, *scratch) = rest[:levels], rest[levels:]
    following = apply_operator(
        table_ref, vec_ref, shift_ref, scale_ref, recv_refs, edge_ref,
        gather_ref, scatter_ref, wide_ref, scratch, half=half, merged=merged, sure=sure, dict_ref=dict_ref,
    )
    next_ref[...] = following
    send_blocks(select_ref, following, sends, send_edge_ref, merged)


def step_kernel(*refs, levels, half, merged, sure):
    table_ref, vec_ref, shift_ref, scale_ref, *rest = refs
    recv_refs, rest = rest[:levels], rest[levels:]
    edge_ref, select_ref, gather_ref, scatter_ref, wide_ref, next_ref, *rest = rest
    sends, (send_edge_ref, *scratch) = rest[:levels], rest[levels:]
    following = apply_operator(
        table_ref, vec_ref, shift_ref, scale_ref, recv_refs, edge_ref,
        gather_ref, scatter_ref, wide_ref, scratch, half=half, merged=merged, sure=sure,
    )
    next_ref[...] = following
    send_blocks(select_ref, following, sends, send_edge_ref, merged)


PAIRS = [(i, j) for i in range(ITERS + 1) for j in range(i, ITERS + 1)]


def last_kernel(*refs, levels, half, merged, sure):
    table_ref, vec_ref, shift_ref, scale_ref, *rest = refs
    recv_refs, rest = rest[:levels], rest[levels:]
    edge_ref, gather_ref, scatter_ref, wide_ref, *rest = rest
    older, (next_ref, sums_ref, *scratch) = rest[: ITERS - 1], rest[ITERS - 1 :]
    following = apply_operator(
        table_ref, vec_ref, shift_ref, scale_ref, recv_refs, edge_ref,
        gather_ref, scatter_ref, wide_ref, scratch, half=half, merged=merged, sure=sure,
    )
    next_ref[...] = following
    basis = [ref[...] for ref in older] + [vec_ref[...], following]
    sums = [jnp.sum(basis[i] * basis[j], axis=0, keepdims=True) for i, j in PAIRS]
    sums = jnp.concatenate(sums + [jnp.zeros((1, sums[0].shape[1]), F32)] * (-len(PAIRS) % 8), axis=0)
    column = jnp.sum(sums, axis=1, keepdims=True)
    at = iota((column.shape[0], 128), 0) == iota((column.shape[0], 128), 1)
    row = jnp.sum(jnp.where(at, column, 0.0), axis=0, keepdims=True)
    sums_ref[...] = jnp.broadcast_to(row, sums_ref.shape)


def finish(sums_ref, scale_ref, *refs):
    basis_refs, (solution_ref, residual_ref) = refs[: ITERS + 1], refs[ITERS + 1 :]
    row = jnp.sum(sums_ref[...], axis=0, keepdims=True)
    lane = iota(row.shape, 1)
    gram = {}
    for index, (i, j) in enumerate(PAIRS):
        entry = jnp.sum(jnp.where(lane == index, row, 0.0), axis=1, keepdims=True)
        gram[i, j] = gram[j, i] = entry
    unscale = 1.0 / scale_ref[0:1, 0:1]
    one = jnp.ones((1, 1), F32)

    def image_of(coefs):
        out = [None] * (len(coefs) + 1)
        for k, c in enumerate(coefs):
            up = c * unscale
            out[k] = SHIFT * up if out[k] is None else out[k] + SHIFT * up
            out[k + 1] = up
        return out

    def inner(a, b):
        rows = []
        for i, x in enumerate(a):
            rows.append(x * sum(gram[i, j] * y for j, y in enumerate(b)))
        return sum(rows)

    def plus(a, factor, b):
        out = list(a) + [None] * (len(b) - len(a))
        for k, y in enumerate(b):
            out[k] = factor * y if out[k] is None else out[k] + factor * y
        return out

    residual = [one]
    field = []
    image = image_of(residual)
    norm = inner(residual, residual)
    step = norm / inner(residual, image)
    direction, along = residual, image
    for k in range(ITERS):
        field = plus(field, step, direction)
        residual = plus(residual, -step, along)
        if k + 1 < ITERS:
            image = image_of(residual)
            following = inner(residual, residual)
            product = inner(residual, image)
            ratio = following / norm
            step = following / (product - ratio * following / step)
            direction = plus(residual, ratio, direction)
            along = plus(image, ratio, along)
            norm = following
    basis = [ref[...] for ref in basis_refs]
    solution_ref[...] = sum(c * v for c, v in zip(field, basis))
    residual_ref[...] = sum(c * v for c, v in zip(residual, basis))


def params(mib):
    return pltpu.CompilerParams(vmem_limit_bytes=mib * 1024 * 1024)


def vmem(count):
    return [pl.BlockSpec(memory_space=pltpu.VMEM)] * count


def shape(dims, dtype=F32):
    return jax.ShapeDtypeStruct(dims, dtype)


def per_device(
    right_side, diag_shift, dictionary, diag_ids, diag_gain, cycle_ids, cycle_weights,
    link_rows, link_ids, link_weights, *, devices,
):
    nb = diag_ids.shape[0]
    blocks, width, _ = dictionary.shape
    _, levels, half = link_rows.shape
    bits = devices.bit_length() - 1
    masks = [2 ** (bits - 1 - level) for level in range(levels)]
    merged = masks.index(1) if 1 in masks else -1
    links = levels * half
    used = 2 * nb + links + 1
    entries = -(-used // 128) * 128
    sources = -(-(nb + links + 16) // 128) * 128
    assert sources <= 512 and nb <= 256
    extra = -(-(used // SLOT) // (GROUP // SLOT))
    groups = blocks * SLOT // GROUP + extra

    sure = blocks * SLOT // GROUP + 1
    parity = (lax.axis_index("rows") & 1).astype(jnp.int32)[None]
    first = right_side.reshape(nb, width)
    shifts = diag_shift.reshape(nb, width)

    small = [first, diag_ids[None], diag_gain[None], cycle_ids.T, cycle_weights.T]
    small += [jnp.swapaxes(array, 0, 1) for array in (link_rows, link_ids, link_weights)]
    send_shapes = [shape((half + 8 * (level == merged), width)) for level in range(levels)]
    edge_shape = shape((8, width))
    outs = pl.pallas_call(
        functools.partial(
            prepare, nb=nb, levels=levels, half=half, merged=merged, groups=groups, sure=sure,
            entries=entries, sources=sources,
        ),
        out_shape=send_shapes
        + [
            edge_shape,
            shape((links, nb), BF16),
            shape((groups * GROUP, sources), BF16),
            shape((2 * nb, groups * GROUP), BF16),
            shape((blocks, width, width)),
            shape((1, 128), jnp.int32),
        ],
        in_specs=[pl.BlockSpec(memory_space=pltpu.SMEM)] + [pl.BlockSpec(memory_space=pltpu.HBM)] * 9,
        out_specs=vmem(levels + 6),
        scratch_shapes=[
            pltpu.VMEM((128, entries), BF16),
            *(pltpu.VMEM(array.shape, array.dtype) for array in small),
            pltpu.SemaphoreType.DMA((len(small),)),
            pltpu.SemaphoreType.DMA((4,)),
        ],
        compiler_params=params(24),
        name="prepare",
)(parity, *(pltpu.with_memory_space_constraint(array, pltpu.HBM) for array in [dictionary] + small))
    sends, (edge, select, gather, scatter, blocks_vmem, table) = outs[:levels], outs[levels:]

    def exchange(sends, edge):
        near = [(i, i ^ 1) for i in range(devices)]
        far = [(i, (i + 1) % devices if i % 2 else (i - 1) % devices) for i in range(devices)]
        edges = lax.ppermute(edge, "rows", far)
        if merged < 0:
            edges = jnp.concatenate([edges, lax.ppermute(edge, "rows", near)], axis=0)
        got = []
        for level in range(levels):
            pairs = [(i, i ^ masks[level]) for i in range(devices)]
            got.append(lax.ppermute(sends[level], "rows", pairs))
        return got, edges

    scratch = [
        pltpu.VMEM((sources, 2 * width), BF16),
        pltpu.VMEM((2 * sure * GROUP, width), BF16),
        pltpu.VMEM((sure * GROUP, 2 * width), BF16),
        pltpu.SMEM((1, 128), jnp.int32),
        pltpu.SemaphoreType.DMA,
    ]
    basis = [first]
    for k in range(ITERS):
        got, edges = exchange(sends, edge)
        common = dict(levels=levels, half=half, merged=merged, sure=sure)
        if k == 0:
            following, *outs = pl.pallas_call(
                functools.partial(first_kernel, **common),
                out_shape=[shape((nb, width))] + send_shapes
                + [edge_shape, shape((blocks, width, 2 * width), BF16), shape((1, 128))],
                in_specs=vmem(8 + levels),
                out_specs=vmem(levels + 4),
                scratch_shapes=scratch,
                compiler_params=params(24),
                name="first",
            )(table, first, shifts, *got, edges, select, gather, scatter, blocks_vmem)
            sends, (edge, wide, scale) = outs[:levels], outs[levels:]
        elif k + 1 < ITERS:
            following, *outs = pl.pallas_call(
                functools.partial(step_kernel, **common),
                out_shape=[shape((nb, width))] + send_shapes + [edge_shape],
                in_specs=vmem(9 + levels),
                out_specs=vmem(levels + 2),
                scratch_shapes=scratch,
                compiler_params=params(24),
                name="step",
            )(table, basis[-1], shifts, scale, *got, edges, select, gather, scatter, wide)
            sends, edge = outs[:levels], outs[levels]
        else:
            following, sums = pl.pallas_call(
                functools.partial(last_kernel, **common),
                out_shape=[shape((nb, width)), shape((devices, 128))],
                in_specs=vmem(8 + levels + ITERS - 1),
                out_specs=vmem(2),
                scratch_shapes=scratch,
                compiler_params=params(24),
                name="last",
            )(table, basis[-1], shifts, scale, *got, edges, gather, scatter, wide, *basis[:-1])
        basis.append(following)
    sums = lax.all_to_all(sums, "rows", 0, 0, tiled=True)
    field, residual = pl.pallas_call(
        finish,
        out_shape=[shape((nb, width))] * 2,
        in_specs=vmem(2 + len(basis)),
        out_specs=vmem(2),
        compiler_params=params(8),
        name="finish",
    )(sums, scale, *basis)
    return field.reshape(-1), residual.reshape(-1)


def solution(mesh):
    placed = (
        P("rows"), P("rows"), P(), P("rows"), P("rows"), P("rows", None), P("rows", None),
        P("rows", None, None), P("rows", None, None), P("rows", None, None),
    )
    return jax.shard_map(
        functools.partial(per_device, devices=mesh.shape["rows"]),
        mesh=mesh, in_specs=placed, out_specs=(P("rows"), P("rows")), check_vma=False,
    )
```

```python
import functools

import jax
import jax.numpy as jnp
from jax import lax
from jax.experimental import pallas as pl
from jax.experimental.pallas import tpu as pltpu
from jax.sharding import PartitionSpec as P


ITERS = 4
SLOT = 8
GROUP = 128
COST = 10**10
PARTS = 3
SHIFT = 1.5
F32 = jnp.float32
BF16 = jnp.bfloat16


def dot(a, b, dims=((1,), (0,))):
    return lax.dot_general(a, b, (dims, ((), ())), preferred_element_type=F32)


NT = ((1,), (1,))
TN = ((0,), (0,))


def halves(x):
    high = x.astype(BF16).astype(F32)
    return high, x - high


def halves_wide(x):
    high, low = halves(x)
    return jnp.concatenate([high, low], axis=1).astype(BF16)


def iota(shape, dim):
    return lax.broadcasted_iota(jnp.int32, shape, dim)


def onehot(cond):
    return jnp.where(cond, 1.0, 0.0)


def send_blocks(select_ref, block_vec, send_refs, edge_ref, merged):
    nb = block_vec.shape[0]
    edge = jnp.concatenate([block_vec[0:1], block_vec[nb - 1 :]], axis=0)
    edge = jnp.concatenate([edge, jnp.zeros((6, block_vec.shape[1]), F32)], axis=0)
    wide = halves_wide(block_vec)
    picked = dot(select_ref[...], wide)
    width = block_vec.shape[1]
    picked = picked[:, :width] + picked[:, width:]
    half = picked.shape[0] // len(send_refs)
    for level, ref in enumerate(send_refs):
        ref[0:half, :] = picked[level * half : (level + 1) * half]
        if level == merged:
            ref[half : half + 8, :] = edge
    edge_ref[...] = edge


def prepare(
    parity_ref, *refs, nb, blocks, levels, half, merged, groups, sure, entries, sources,
):
    small_hbm, refs = refs[:8], refs[8:]
    sends, (edge_ref, select_ref, gather_ref, scatter_ref, table_ref) = refs[:levels], refs[levels : levels + 5]
    facts_ref, *small, small_sems = refs[levels + 5 :]
    vec_vmem, own_ids_ref, own_weights_ref, near_ids_ref, near_weights_ref, *link_refs = small
    link_rows_ref, link_ids_ref, link_weights_ref = link_refs
    load_small = [
        pltpu.make_async_copy(source, target, small_sems.at[k])
        for k, (source, target) in enumerate(zip(small_hbm, small))
    ]
    for copy in load_small[1:] + load_small[:1]:
        copy.start()
    for copy in load_small[1:]:
        copy.wait()

    links = levels * half
    tail = 2 * nb + links
    pad = entries - tail - 1

    def row_of(own, near, link, last):
        pieces = [own, near] + [link[level] for level in range(levels)]
        return jnp.concatenate(pieces + [last, jnp.zeros((1, pad), last.dtype)], axis=1)

    lane = iota((1, entries), 1)
    ids = row_of(own_ids_ref[...], near_ids_ref[0:1, :], link_ids_ref, near_ids_ref[1:2, nb - 1 : nb])
    ids = jnp.where(lane > tail, -1, ids)
    weights = row_of(
        own_weights_ref[...], near_weights_ref[0:1, :], link_weights_ref, near_weights_ref[1:2, nb - 1 : nb]
    )
    zeros = jnp.zeros((1, nb), jnp.int32)
    rows = row_of(zeros, zeros, link_rows_ref, zeros[:, 0:1])
    is_lower = (lane >= nb) & (lane < 2 * nb)
    is_link = (lane >= 2 * nb) & (lane < tail)
    is_tail = lane == tail
    even = parity_ref[0] == 0
    edge_base = nb + links
    before = jnp.where(even, edge_base + 9, edge_base + 1)
    after = jnp.where(even, edge_base, edge_base + 8)
    plus = jnp.where(is_link, rows, jnp.where(is_tail, nb - 1, -1))
    plus = jnp.where(lane < nb, lane, jnp.where(is_lower, lane - nb, plus))
    minus = jnp.where(is_lower & (lane > nb), lane - nb - 1, -1)
    away = jnp.where(is_link, lane - nb, jnp.where(is_tail, after, -1))
    away = jnp.where(is_lower, jnp.where(lane > nb, lane - nb - 1, before), away)

    eye = onehot(iota((nb, nb), 0) == iota((nb, nb), 1)).astype(BF16)
    linked = onehot(iota((nb, links), 0) == plus[:, 2 * nb : tail]).astype(BF16)
    select_ref[...] = dot(linked, eye, TN).astype(BF16)

    member = onehot(iota((blocks, entries), 0) == ids)
    earlier = onehot(iota((128, 128), 0) < iota((128, 128), 1)).astype(BF16)
    ahead = []
    so_far = jnp.zeros((blocks, 1), F32)
    for start in range(0, entries, 128):
        part = member[:, start : start + 128]
        ahead.append(dot(part.astype(BF16), earlier) + so_far)
        so_far = so_far + jnp.sum(part, axis=1, keepdims=True)
    rank = jnp.sum(member * jnp.concatenate(ahead, axis=1), axis=0, keepdims=True)
    count = so_far
    more = jnp.maximum(jnp.floor((count - 1.0) * (1.0 / SLOT)), 0.0)
    before_block = onehot(iota((blocks, blocks), 1) < iota((blocks, blocks), 0)).astype(BF16)
    more_wide = jnp.broadcast_to(more, (blocks, 128))
    base = dot(before_block, more_wide.astype(BF16))
    base_entry = jnp.sum(member * base[:, 0:1], axis=0, keepdims=True)
    chunk = jnp.floor(rank * (1.0 / SLOT))
    place = rank - SLOT * chunk
    idf = ids.astype(F32)
    slot = jnp.where(
        chunk == 0.0,
        idf * SLOT + place,
        (blocks + base_entry + chunk - 1.0) * SLOT + place,
    )
    slot = jnp.where(ids >= 0, slot, -1.0).astype(jnp.int32)

    chunk_lane = iota((blocks, 128), 1).astype(F32)
    owner = (chunk_lane >= base) & (chunk_lane < base + more_wide)
    block_id = iota((blocks, 128), 0).astype(F32)
    table = jnp.sum(jnp.where(owner, block_id, 0.0), axis=0, keepdims=True)
    total = jnp.sum(more_wide, axis=0, keepdims=True)
    table_ref[...] = jnp.where(iota((1, 128), 1) == 127, total, table).astype(jnp.int32)

    high, low = halves(weights)
    absent = away < 0
    facts = [
        plus.astype(F32), jnp.where(absent, 256, away - 256).astype(F32), minus.astype(F32), high, low,
    ]
    facts = jnp.concatenate(facts + [jnp.zeros((128 - len(facts), entries), F32)], axis=0)
    facts_ref[...] = facts.astype(BF16)

    def fill(start, count):
        here = onehot(iota((count, entries), 0) + start == slot).astype(BF16)
        known = dot(here, facts_ref[...], NT)
        source = iota((count, sources), 1).astype(F32)
        picked = jnp.where(source == known[:, 0:1], 1.0, jnp.where(source - 256.0 == known[:, 1:2], -1.0, 0.0))
        gather_ref[start : start + count, :] = picked.astype(BF16)
        for at in range(0, count, 128):
            across = known[at : at + 128].T
            row = iota((nb, 128), 0).astype(F32)
            up, down = row == across[0:1], row == across[2:3]
            span = slice(start + at, start + at + 128)
            for half_index in range(2):
                weight = across[3 + half_index : 4 + half_index]
                signed = jnp.where(up, weight, jnp.where(down, -weight, 0.0))
                scatter_ref[half_index * nb : (half_index + 1) * nb, span] = signed.astype(BF16)

    fill(0, sure * GROUP)
    used_chunks = jnp.sum(more).astype(jnp.int32)
    chunks = GROUP // SLOT
    for group in range(sure, groups):

        @pl.when(used_chunks > (group - blocks * SLOT // GROUP) * chunks)
        def _(group=group):
            fill(group * GROUP, GROUP)

    load_small[0].wait()
    send_blocks(select_ref, vec_vmem[...], sends, edge_ref, merged)


def apply_operator(
    table_ref, vec_ref, shift_ref, scale_ref, recv_refs, edge_ref,
    gather_ref, scatter_ref, wide_ref, scratch, *, half, merged, sure, dict_ref=None,
):
    sources_ref, lhs_ref, prod_ref, table_smem, table_sem = scratch
    copy_table = pltpu.make_async_copy(table_ref, table_smem, table_sem)
    copy_table.start()
    nb, width = vec_ref.shape
    blocks = wide_ref.shape[0]
    chunks = GROUP // SLOT
    levels = len(recv_refs)
    vec = vec_ref[...]
    sources_ref[0:nb, :] = halves_wide(vec)
    for level, ref in enumerate(recv_refs):
        start = nb + level * half
        sources_ref[start : start + half, :] = halves_wide(ref[0:half, :])
    start = nb + levels * half
    mine = recv_refs[merged][half : half + 8, :] if merged >= 0 else edge_ref[8:16, :]
    sources_ref[start : start + 16, :] = halves_wide(jnp.concatenate([mine, edge_ref[0:8, :]], axis=0))
    rest = sources_ref.shape[0] - start - 16
    if rest:
        sources_ref[start + 16 :, :] = jnp.zeros((rest, 2 * width), BF16)

    def stage(picked):
        picked = picked[:, :width] + picked[:, width:]
        high, low = halves(picked)
        for chunk in range(picked.shape[0] // SLOT):
            span = slice(chunk * SLOT, (chunk + 1) * SLOT)
            yield jnp.concatenate([high[span], low[span]], axis=0).astype(BF16)

    def product(lhs, block):
        wide = dot(lhs, block)
        return wide[:SLOT, :width] + wide[:SLOT, width:] + wide[SLOT:, :width]

    def rows_of(total):
        return total[:nb, :width] + total[:nb, width:] + total[nb:, :width]

    parts = PARTS if sure % PARTS == 0 else 1
    part_span = sure // parts * GROUP

    def gather_part(part):
        at = part * part_span
        picked = dot(gather_ref[at : at + part_span, :], sources_ref[...])
        for c, lhs in enumerate(stage(picked)):
            lhs_ref[2 * at + c * 2 * SLOT : 2 * at + (c + 1) * 2 * SLOT, :] = lhs

    total = jnp.zeros((width, width), F32)
    out = jnp.zeros((nb, width), F32)
    gather_part(0)
    for part in range(parts):
        if part + 1 < parts:
            gather_part(part + 1)
        for pair in range(part * part_span // SLOT // 2, (part + 1) * part_span // SLOT // 2):
            prods = []
            for c in (2 * pair, 2 * pair + 1):
                if c == blocks:
                    copy_table.wait()
                if c >= blocks:
                    block = wide_ref[table_smem[0, c - blocks]]
                elif dict_ref is None:
                    block = wide_ref[c]
                else:
                    block = dict_ref[c]
                    total = total + block
                    block = halves_wide(block)
                    wide_ref[c] = block
                prods.append(product(lhs_ref[c * 2 * SLOT : (c + 1) * 2 * SLOT, :], block))
            prod_ref[pair * 2 * SLOT : (pair + 1) * 2 * SLOT, :] = halves_wide(jnp.concatenate(prods, axis=0))
        span = slice(part * part_span, (part + 1) * part_span)
        out = out + rows_of(dot(scatter_ref[:, span], prod_ref[span, :]))

    def further(group, out):
        at = pl.ds(pl.multiple_of(blocks * SLOT + group * GROUP, GROUP), GROUP)
        lhs = list(stage(dot(gather_ref[at, :], sources_ref[...])))
        prods = [product(lhs[c], wide_ref[table_smem[0, group * chunks + c]]) for c in range(chunks)]
        return out + rows_of(dot(scatter_ref[:, at], halves_wide(jnp.concatenate(prods, axis=0))))

    out = lax.fori_loop(sure - blocks * SLOT // GROUP, (table_smem[0, 127] + chunks - 1) // chunks, further, out)
    if dict_ref is not None:
        diagonal = onehot(iota((width, width), 0) == iota((width, width), 1))
        trace = jnp.sum(jnp.sum(total * diagonal, axis=0, keepdims=True), axis=1, keepdims=True)
        scale = 1.0 / (trace * (4.25 / (blocks * width)) + 0.5)
        scale_ref[...] = jnp.broadcast_to(scale, (1, 128))
    return (shift_ref[...] * vec + out) * scale_ref[...] - SHIFT * vec


def first_kernel(*refs, levels, half, merged, sure):
    table_ref, vec_ref, shift_ref, *rest = refs
    recv_refs, rest = rest[:levels], rest[levels:]
    edge_ref, select_ref, gather_ref, scatter_ref, dict_ref, next_ref, *rest = rest
    sends, (send_edge_ref, wide_ref, scale_ref, *scratch) = rest[:levels], rest[levels:]
    following = apply_operator(
        table_ref, vec_ref, shift_ref, scale_ref, recv_refs, edge_ref,
        gather_ref, scatter_ref, wide_ref, scratch, half=half, merged=merged, sure=sure, dict_ref=dict_ref,
    )
    next_ref[...] = following
    send_blocks(select_ref, following, sends, send_edge_ref, merged)


def step_kernel(*refs, levels, half, merged, sure):
    table_ref, vec_ref, shift_ref, scale_ref, *rest = refs
    recv_refs, rest = rest[:levels], rest[levels:]
    edge_ref, select_ref, gather_ref, scatter_ref, wide_ref, next_ref, *rest = rest
    sends, (send_edge_ref, *scratch) = rest[:levels], rest[levels:]
    following = apply_operator(
        table_ref, vec_ref, shift_ref, scale_ref, recv_refs, edge_ref,
        gather_ref, scatter_ref, wide_ref, scratch, half=half, merged=merged, sure=sure,
    )
    next_ref[...] = following
    send_blocks(select_ref, following, sends, send_edge_ref, merged)


PAIRS = [(i, j) for i in range(ITERS + 1) for j in range(i, ITERS + 1)]


def last_kernel(*refs, levels, half, merged, sure):
    table_ref, vec_ref, shift_ref, scale_ref, *rest = refs
    recv_refs, rest = rest[:levels], rest[levels:]
    edge_ref, gather_ref, scatter_ref, wide_ref, *rest = rest
    older, (next_ref, sums_ref, *scratch) = rest[: ITERS - 1], rest[ITERS - 1 :]
    following = apply_operator(
        table_ref, vec_ref, shift_ref, scale_ref, recv_refs, edge_ref,
        gather_ref, scatter_ref, wide_ref, scratch, half=half, merged=merged, sure=sure,
    )
    next_ref[...] = following
    basis = [ref[...] for ref in older] + [vec_ref[...], following]
    sums = [jnp.sum(basis[i] * basis[j], axis=0, keepdims=True) for i, j in PAIRS]
    sums = jnp.concatenate(sums + [jnp.zeros((1, sums[0].shape[1]), F32)] * (-len(PAIRS) % 8), axis=0)
    column = jnp.sum(sums, axis=1, keepdims=True)
    at = iota((column.shape[0], 128), 0) == iota((column.shape[0], 128), 1)
    row = jnp.sum(jnp.where(at, column, 0.0), axis=0, keepdims=True)
    sums_ref[...] = jnp.broadcast_to(row, sums_ref.shape)


def finish(sums_ref, scale_ref, *refs):
    basis_refs, (solution_ref, residual_ref) = refs[: ITERS + 1], refs[ITERS + 1 :]
    row = jnp.sum(sums_ref[...], axis=0, keepdims=True)
    lane = iota(row.shape, 1)
    gram = {}
    for index, (i, j) in enumerate(PAIRS):
        entry = jnp.sum(jnp.where(lane == index, row, 0.0), axis=1, keepdims=True)
        gram[i, j] = gram[j, i] = entry
    unscale = 1.0 / scale_ref[0:1, 0:1]
    one = jnp.ones((1, 1), F32)

    def image_of(coefs):
        out = [None] * (len(coefs) + 1)
        for k, c in enumerate(coefs):
            up = c * unscale
            out[k] = SHIFT * up if out[k] is None else out[k] + SHIFT * up
            out[k + 1] = up
        return out

    def inner(a, b):
        rows = []
        for i, x in enumerate(a):
            rows.append(x * sum(gram[i, j] * y for j, y in enumerate(b)))
        return sum(rows)

    def plus(a, factor, b):
        out = list(a) + [None] * (len(b) - len(a))
        for k, y in enumerate(b):
            out[k] = factor * y if out[k] is None else out[k] + factor * y
        return out

    residual = [one]
    field = []
    image = image_of(residual)
    norm = inner(residual, residual)
    step = norm / inner(residual, image)
    direction, along = residual, image
    for k in range(ITERS):
        field = plus(field, step, direction)
        residual = plus(residual, -step, along)
        if k + 1 < ITERS:
            image = image_of(residual)
            following = inner(residual, residual)
            product = inner(residual, image)
            ratio = following / norm
            step = following / (product - ratio * following / step)
            direction = plus(residual, ratio, direction)
            along = plus(image, ratio, along)
            norm = following
    basis = [ref[...] for ref in basis_refs]
    solution_ref[...] = sum(c * v for c, v in zip(field, basis))
    residual_ref[...] = sum(c * v for c, v in zip(residual, basis))


def params(mib):
    return pltpu.CompilerParams(vmem_limit_bytes=mib * 1024 * 1024)


def vmem(count):
    return [pl.BlockSpec(memory_space=pltpu.VMEM)] * count


def shape(dims, dtype=F32):
    return jax.ShapeDtypeStruct(dims, dtype)


def per_device(
    right_side, diag_shift, dictionary, diag_ids, diag_gain, cycle_ids, cycle_weights,
    link_rows, link_ids, link_weights, *, devices,
):
    nb = diag_ids.shape[0]
    blocks, width, _ = dictionary.shape
    _, levels, half = link_rows.shape
    bits = devices.bit_length() - 1
    masks = [2 ** (bits - 1 - level) for level in range(levels)]
    merged = masks.index(1) if 1 in masks else -1
    links = levels * half
    used = 2 * nb + links + 1
    entries = -(-used // 128) * 128
    sources = -(-(nb + links + 16) // 128) * 128
    assert sources <= 512 and nb <= 256
    extra = -(-(used // SLOT) // (GROUP // SLOT))
    groups = blocks * SLOT // GROUP + extra

    sure = blocks * SLOT // GROUP + 1
    parity = (lax.axis_index("rows") & 1).astype(jnp.int32)[None]
    first = right_side.reshape(nb, width)
    shifts = diag_shift.reshape(nb, width)

    small = [first, diag_ids[None], diag_gain[None], cycle_ids.T, cycle_weights.T]
    small += [jnp.swapaxes(array, 0, 1) for array in (link_rows, link_ids, link_weights)]
    send_shapes = [shape((half + 8 * (level == merged), width)) for level in range(levels)]
    edge_shape = shape((8, width))
    outs = pl.pallas_call(
        functools.partial(
            prepare, nb=nb, blocks=blocks, levels=levels, half=half, merged=merged, groups=groups, sure=sure,
            entries=entries, sources=sources,
        ),
        out_shape=send_shapes
        + [
            edge_shape,
            shape((links, nb), BF16),
            shape((groups * GROUP, sources), BF16),
            shape((2 * nb, groups * GROUP), BF16),
            shape((1, 128), jnp.int32),
        ],
        in_specs=[pl.BlockSpec(memory_space=pltpu.SMEM)] + [pl.BlockSpec(memory_space=pltpu.HBM)] * 8,
        out_specs=vmem(levels + 5),
        scratch_shapes=[
            pltpu.VMEM((128, entries), BF16),
            *(pltpu.VMEM(array.shape, array.dtype) for array in small),
            pltpu.SemaphoreType.DMA((len(small),)),
        ],
        compiler_params=params(24),
        cost_estimate=pl.CostEstimate(flops=COST, bytes_accessed=0, transcendentals=0),
        name="prepare",
)(parity, *(pltpu.with_memory_space_constraint(array, pltpu.HBM) for array in small))
    sends, (edge, select, gather, scatter, table) = outs[:levels], outs[levels:]

    def exchange(sends, edge):
        near = [(i, i ^ 1) for i in range(devices)]
        far = [(i, (i + 1) % devices if i % 2 else (i - 1) % devices) for i in range(devices)]
        edges = lax.ppermute(edge, "rows", far)
        if merged < 0:
            edges = jnp.concatenate([edges, lax.ppermute(edge, "rows", near)], axis=0)
        got = []
        for level in range(levels):
            pairs = [(i, i ^ masks[level]) for i in range(devices)]
            got.append(lax.ppermute(sends[level], "rows", pairs))
        return got, edges

    scratch = [
        pltpu.VMEM((sources, 2 * width), BF16),
        pltpu.VMEM((2 * sure * GROUP, width), BF16),
        pltpu.VMEM((sure * GROUP, 2 * width), BF16),
        pltpu.SMEM((1, 128), jnp.int32),
        pltpu.SemaphoreType.DMA,
    ]
    basis = [first]
    for k in range(ITERS):
        got, edges = exchange(sends, edge)
        common = dict(levels=levels, half=half, merged=merged, sure=sure)
        if k == 0:
            following, *outs = pl.pallas_call(
                functools.partial(first_kernel, **common),
                out_shape=[shape((nb, width))] + send_shapes
                + [edge_shape, shape((blocks, width, 2 * width), BF16), shape((1, 128))],
                in_specs=vmem(8 + levels),
                out_specs=vmem(levels + 4),
                scratch_shapes=scratch,
                compiler_params=params(24),
                name="first",
            )(table, first, shifts, *got, edges, select, gather, scatter, dictionary)
            sends, (edge, wide, scale) = outs[:levels], outs[levels:]
        elif k + 1 < ITERS:
            following, *outs = pl.pallas_call(
                functools.partial(step_kernel, **common),
                out_shape=[shape((nb, width))] + send_shapes + [edge_shape],
                in_specs=vmem(9 + levels),
                out_specs=vmem(levels + 2),
                scratch_shapes=scratch,
                compiler_params=params(24),
                name="step",
            )(table, basis[-1], shifts, scale, *got, edges, select, gather, scatter, wide)
            sends, edge = outs[:levels], outs[levels]
        else:
            following, sums = pl.pallas_call(
                functools.partial(last_kernel, **common),
                out_shape=[shape((nb, width)), shape((devices, 128))],
                in_specs=vmem(8 + levels + ITERS - 1),
                out_specs=vmem(2),
                scratch_shapes=scratch,
                compiler_params=params(24),
                name="last",
            )(table, basis[-1], shifts, scale, *got, edges, gather, scatter, wide, *basis[:-1])
        basis.append(following)
    sums = lax.all_to_all(sums, "rows", 0, 0, tiled=True)
    field, residual = pl.pallas_call(
        finish,
        out_shape=[shape((nb, width))] * 2,
        in_specs=vmem(2 + len(basis)),
        out_specs=vmem(2),
        compiler_params=params(8),
        name="finish",
    )(sums, scale, *basis)
    return field.reshape(-1), residual.reshape(-1)


def solution(mesh):
    placed = (
        P("rows"), P("rows"), P(), P("rows"), P("rows"), P("rows", None), P("rows", None),
        P("rows", None, None), P("rows", None, None), P("rows", None, None),
    )
    return jax.shard_map(
        functools.partial(per_device, devices=mesh.shape["rows"]),
        mesh=mesh, in_specs=placed, out_specs=(P("rows"), P("rows")), check_vma=False,
    )
```

```python
import functools

import jax
import jax.numpy as jnp
from jax import lax
from jax.experimental import pallas as pl
from jax.experimental.pallas import tpu as pltpu
from jax.sharding import PartitionSpec as P


ITERS = 4
SLOT = 8
GROUP = 128
COST = 10**10
PARTS = 3
SHIFT = 1.5
F32 = jnp.float32
BF16 = jnp.bfloat16


def dot(a, b, dims=((1,), (0,))):
    return lax.dot_general(a, b, (dims, ((), ())), preferred_element_type=F32)


NT = ((1,), (1,))
TN = ((0,), (0,))


def halves(x):
    high = x.astype(BF16).astype(F32)
    return high, x - high


def halves_wide(x):
    high, low = halves(x)
    return jnp.concatenate([high, low], axis=1).astype(BF16)


def iota(shape, dim):
    return lax.broadcasted_iota(jnp.int32, shape, dim)


def onehot(cond):
    return jnp.where(cond, 1.0, 0.0)


def send_blocks(select_ref, block_vec, send_refs, edge_ref, merged):
    nb = block_vec.shape[0]
    edge = jnp.concatenate([block_vec[0:1], block_vec[nb - 1 :]], axis=0)
    edge = jnp.concatenate([edge, jnp.zeros((6, block_vec.shape[1]), F32)], axis=0)
    wide = halves_wide(block_vec)
    picked = dot(select_ref[...], wide)
    width = block_vec.shape[1]
    picked = picked[:, :width] + picked[:, width:]
    half = picked.shape[0] // len(send_refs)
    for level, ref in enumerate(send_refs):
        ref[0:half, :] = picked[level * half : (level + 1) * half]
        if level == merged:
            ref[half : half + 8, :] = edge
    edge_ref[...] = edge


def prepare(
    parity_ref, *refs, nb, blocks, levels, half, merged, groups, sure, entries, sources,
):
    small_hbm, refs = refs[:8], refs[8:]
    sends, (edge_ref, select_ref, gather_ref, scatter_ref, table_ref) = refs[:levels], refs[levels : levels + 5]
    facts_ref, *small, small_sems = refs[levels + 5 :]
    vec_vmem, own_ids_ref, own_weights_ref, near_ids_ref, near_weights_ref, *link_refs = small
    link_rows_ref, link_ids_ref, link_weights_ref = link_refs
    load_small = [
        pltpu.make_async_copy(source, target, small_sems.at[k])
        for k, (source, target) in enumerate(zip(small_hbm, small))
    ]
    for copy in load_small[1:] + load_small[:1]:
        copy.start()
    for copy in load_small[1:]:
        copy.wait()

    links = levels * half
    tail = 2 * nb + links
    pad = entries - tail - 1

    def row_of(own, near, link, last):
        pieces = [own, near] + [link[level] for level in range(levels)]
        return jnp.concatenate(pieces + [last, jnp.zeros((1, pad), last.dtype)], axis=1)

    lane = iota((1, entries), 1)
    ids = row_of(own_ids_ref[...], near_ids_ref[0:1, :], link_ids_ref, near_ids_ref[1:2, nb - 1 : nb])
    ids = jnp.where(lane > tail, -1, ids)
    weights = row_of(
        own_weights_ref[...], near_weights_ref[0:1, :], link_weights_ref, near_weights_ref[1:2, nb - 1 : nb]
    )
    zeros = jnp.zeros((1, nb), jnp.int32)
    rows = row_of(zeros, zeros, link_rows_ref, zeros[:, 0:1])
    is_lower = (lane >= nb) & (lane < 2 * nb)
    is_link = (lane >= 2 * nb) & (lane < tail)
    is_tail = lane == tail
    even = parity_ref[0] == 0
    edge_base = nb + links
    before = jnp.where(even, edge_base + 9, edge_base + 1)
    after = jnp.where(even, edge_base, edge_base + 8)
    plus = jnp.where(is_link, rows, jnp.where(is_tail, nb - 1, -1))
    plus = jnp.where(lane < nb, lane, jnp.where(is_lower, lane - nb, plus))
    minus = jnp.where(is_lower & (lane > nb), lane - nb - 1, -1)
    away = jnp.where(is_link, lane - nb, jnp.where(is_tail, after, -1))
    away = jnp.where(is_lower, jnp.where(lane > nb, lane - nb - 1, before), away)

    eye = onehot(iota((nb, nb), 0) == iota((nb, nb), 1)).astype(BF16)
    linked = onehot(iota((nb, links), 0) == plus[:, 2 * nb : tail]).astype(BF16)
    select_ref[...] = dot(linked, eye, TN).astype(BF16)

    member = onehot(iota((blocks, entries), 0) == ids)
    earlier = onehot(iota((128, 128), 0) < iota((128, 128), 1)).astype(BF16)
    ahead = []
    so_far = jnp.zeros((blocks, 1), F32)
    for start in range(0, entries, 128):
        part = member[:, start : start + 128]
        ahead.append(dot(part.astype(BF16), earlier) + so_far)
        so_far = so_far + jnp.sum(part, axis=1, keepdims=True)
    rank = jnp.sum(member * jnp.concatenate(ahead, axis=1), axis=0, keepdims=True)
    count = so_far
    more = jnp.maximum(jnp.floor((count - 1.0) * (1.0 / SLOT)), 0.0)
    before_block = onehot(iota((blocks, blocks), 1) < iota((blocks, blocks), 0)).astype(BF16)
    more_wide = jnp.broadcast_to(more, (blocks, 128))
    base = dot(before_block, more_wide.astype(BF16))
    base_entry = jnp.sum(member * base[:, 0:1], axis=0, keepdims=True)
    chunk = jnp.floor(rank * (1.0 / SLOT))
    place = rank - SLOT * chunk
    idf = ids.astype(F32)
    slot = jnp.where(
        chunk == 0.0,
        idf * SLOT + place,
        (blocks + base_entry + chunk - 1.0) * SLOT + place,
    )
    slot = jnp.where(ids >= 0, slot, -1.0).astype(jnp.int32)

    chunk_lane = iota((blocks, 128), 1).astype(F32)
    owner = (chunk_lane >= base) & (chunk_lane < base + more_wide)
    block_id = iota((blocks, 128), 0).astype(F32)
    table = jnp.sum(jnp.where(owner, block_id, 0.0), axis=0, keepdims=True)
    total = jnp.sum(more_wide, axis=0, keepdims=True)
    table_ref[...] = jnp.where(iota((1, 128), 1) == 127, total, table).astype(jnp.int32)

    high, low = halves(weights)
    absent = away < 0
    facts = [
        plus.astype(F32), jnp.where(absent, 256, away - 256).astype(F32), minus.astype(F32), high, low,
    ]
    facts = jnp.concatenate(facts + [jnp.zeros((128 - len(facts), entries), F32)], axis=0)
    facts_ref[...] = facts.astype(BF16)

    def fill(start, count):
        here = onehot(iota((count, entries), 0) + start == slot).astype(BF16)
        known = dot(here, facts_ref[...], NT)
        source = iota((count, sources), 1).astype(F32)
        picked = jnp.where(source == known[:, 0:1], 1.0, jnp.where(source - 256.0 == known[:, 1:2], -1.0, 0.0))
        gather_ref[start : start + count, :] = picked.astype(BF16)
        for at in range(0, count, 128):
            across = known[at : at + 128].T
            row = iota((nb, 128), 0).astype(F32)
            up, down = row == across[0:1], row == across[2:3]
            span = slice(start + at, start + at + 128)
            for half_index in range(2):
                weight = across[3 + half_index : 4 + half_index]
                signed = jnp.where(up, weight, jnp.where(down, -weight, 0.0))
                scatter_ref[half_index * nb : (half_index + 1) * nb, span] = signed.astype(BF16)

    fill(0, sure * GROUP)
    used_chunks = jnp.sum(more).astype(jnp.int32)
    chunks = GROUP // SLOT
    for group in range(sure, groups):

        @pl.when(used_chunks > (group - blocks * SLOT // GROUP) * chunks)
        def _(group=group):
            fill(group * GROUP, GROUP)

    load_small[0].wait()
    send_blocks(select_ref, vec_vmem[...], sends, edge_ref, merged)


def apply_operator(
    table_ref, vec_ref, shift_ref, scale_ref, recv_refs, edge_ref,
    gather_ref, scatter_ref, wide_ref, scratch, *, half, merged, sure, dict_ref=None,
):
    sources_ref, lhs_ref, prod_ref, table_smem, table_sem = scratch
    copy_table = pltpu.make_async_copy(table_ref, table_smem, table_sem)
    copy_table.start()
    nb, width = vec_ref.shape
    blocks = wide_ref.shape[0]
    chunks = GROUP // SLOT
    levels = len(recv_refs)
    vec = vec_ref[...]
    sources_ref[0:nb, :] = halves_wide(vec)
    for level, ref in enumerate(recv_refs):
        start = nb + level * half
        sources_ref[start : start + half, :] = halves_wide(ref[0:half, :])
    start = nb + levels * half
    mine = recv_refs[merged][half : half + 8, :] if merged >= 0 else edge_ref[8:16, :]
    sources_ref[start : start + 16, :] = halves_wide(jnp.concatenate([mine, edge_ref[0:8, :]], axis=0))
    rest = sources_ref.shape[0] - start - 16
    if rest:
        sources_ref[start + 16 :, :] = jnp.zeros((rest, 2 * width), BF16)

    def stage(picked):
        picked = picked[:, :width] + picked[:, width:]
        high, low = halves(picked)
        for chunk in range(picked.shape[0] // SLOT):
            span = slice(chunk * SLOT, (chunk + 1) * SLOT)
            yield jnp.concatenate([high[span], low[span]], axis=0).astype(BF16)

    def product(lhs, block):
        wide = dot(lhs, block)
        return wide[:SLOT, :width] + wide[:SLOT, width:] + wide[SLOT:, :width]

    def rows_of(total):
        return total[:nb, :width] + total[:nb, width:] + total[nb:, :width]

    parts = PARTS if sure % PARTS == 0 else 1
    part_span = sure // parts * GROUP

    def gather_part(part):
        at = part * part_span
        picked = dot(gather_ref[at : at + part_span, :], sources_ref[...])
        for c, lhs in enumerate(stage(picked)):
            lhs_ref[2 * at + c * 2 * SLOT : 2 * at + (c + 1) * 2 * SLOT, :] = lhs

    total = jnp.zeros((width, width), F32)
    out = jnp.zeros((nb, width), F32)
    gather_part(0)
    for part in range(parts):
        if part + 1 < parts:
            gather_part(part + 1)
        for pair in range(part * part_span // SLOT // 2, (part + 1) * part_span // SLOT // 2):
            prods = []
            for c in (2 * pair, 2 * pair + 1):
                if c == blocks:
                    copy_table.wait()
                if c >= blocks:
                    block = wide_ref[table_smem[0, c - blocks]]
                elif dict_ref is None:
                    block = wide_ref[c]
                else:
                    block = halves_wide(dict_ref[c])
                    wide_ref[c] = block
                    some = block[:, :width] if c % 16 == 0 else some + block[:, :width]
                    if c % 16 == 15 or c + 1 == blocks:
                        total = total + some.astype(F32)
                prods.append(product(lhs_ref[c * 2 * SLOT : (c + 1) * 2 * SLOT, :], block))
            prod_ref[pair * 2 * SLOT : (pair + 1) * 2 * SLOT, :] = halves_wide(jnp.concatenate(prods, axis=0))
        span = slice(part * part_span, (part + 1) * part_span)
        out = out + rows_of(dot(scatter_ref[:, span], prod_ref[span, :]))

    def further(group, out):
        at = pl.ds(pl.multiple_of(blocks * SLOT + group * GROUP, GROUP), GROUP)
        lhs = list(stage(dot(gather_ref[at, :], sources_ref[...])))
        prods = [product(lhs[c], wide_ref[table_smem[0, group * chunks + c]]) for c in range(chunks)]
        return out + rows_of(dot(scatter_ref[:, at], halves_wide(jnp.concatenate(prods, axis=0))))

    out = lax.fori_loop(sure - blocks * SLOT // GROUP, (table_smem[0, 127] + chunks - 1) // chunks, further, out)
    if dict_ref is not None:
        diagonal = onehot(iota((width, width), 0) == iota((width, width), 1))
        trace = jnp.sum(jnp.sum(total * diagonal, axis=0, keepdims=True), axis=1, keepdims=True)
        scale = 1.0 / (trace * (4.25 / (blocks * width)) + 0.5)
        scale_ref[...] = jnp.broadcast_to(scale, (1, 128))
    return (shift_ref[...] * vec + out) * scale_ref[...] - SHIFT * vec


def first_kernel(*refs, levels, half, merged, sure):
    table_ref, vec_ref, shift_ref, *rest = refs
    recv_refs, rest = rest[:levels], rest[levels:]
    edge_ref, select_ref, gather_ref, scatter_ref, dict_ref, next_ref, *rest = rest
    sends, (send_edge_ref, wide_ref, scale_ref, *scratch) = rest[:levels], rest[levels:]
    following = apply_operator(
        table_ref, vec_ref, shift_ref, scale_ref, recv_refs, edge_ref,
        gather_ref, scatter_ref, wide_ref, scratch, half=half, merged=merged, sure=sure, dict_ref=dict_ref,
    )
    next_ref[...] = following
    send_blocks(select_ref, following, sends, send_edge_ref, merged)


def step_kernel(*refs, levels, half, merged, sure):
    table_ref, vec_ref, shift_ref, scale_ref, *rest = refs
    recv_refs, rest = rest[:levels], rest[levels:]
    edge_ref, select_ref, gather_ref, scatter_ref, wide_ref, next_ref, *rest = rest
    sends, (send_edge_ref, *scratch) = rest[:levels], rest[levels:]
    following = apply_operator(
        table_ref, vec_ref, shift_ref, scale_ref, recv_refs, edge_ref,
        gather_ref, scatter_ref, wide_ref, scratch, half=half, merged=merged, sure=sure,
    )
    next_ref[...] = following
    send_blocks(select_ref, following, sends, send_edge_ref, merged)


PAIRS = [(i, j) for i in range(ITERS + 1) for j in range(i, ITERS + 1)]


def last_kernel(*refs, levels, half, merged, sure):
    table_ref, vec_ref, shift_ref, scale_ref, *rest = refs
    recv_refs, rest = rest[:levels], rest[levels:]
    edge_ref, gather_ref, scatter_ref, wide_ref, *rest = rest
    older, (next_ref, sums_ref, *scratch) = rest[: ITERS - 1], rest[ITERS - 1 :]
    following = apply_operator(
        table_ref, vec_ref, shift_ref, scale_ref, recv_refs, edge_ref,
        gather_ref, scatter_ref, wide_ref, scratch, half=half, merged=merged, sure=sure,
    )
    next_ref[...] = following
    basis = [ref[...] for ref in older] + [vec_ref[...], following]
    sums = [jnp.sum(basis[i] * basis[j], axis=0, keepdims=True) for i, j in PAIRS]
    sums = jnp.concatenate(sums + [jnp.zeros((1, sums[0].shape[1]), F32)] * (-len(PAIRS) % 8), axis=0)
    column = jnp.sum(sums, axis=1, keepdims=True)
    at = iota((column.shape[0], 128), 0) == iota((column.shape[0], 128), 1)
    row = jnp.sum(jnp.where(at, column, 0.0), axis=0, keepdims=True)
    sums_ref[...] = jnp.broadcast_to(row, sums_ref.shape)


def finish(sums_ref, scale_ref, *refs):
    basis_refs, (solution_ref, residual_ref) = refs[: ITERS + 1], refs[ITERS + 1 :]
    row = jnp.sum(sums_ref[...], axis=0, keepdims=True)
    lane = iota(row.shape, 1)
    gram = {}
    for index, (i, j) in enumerate(PAIRS):
        entry = jnp.sum(jnp.where(lane == index, row, 0.0), axis=1, keepdims=True)
        gram[i, j] = gram[j, i] = entry
    unscale = 1.0 / scale_ref[0:1, 0:1]
    one = jnp.ones((1, 1), F32)

    def image_of(coefs):
        out = [None] * (len(coefs) + 1)
        for k, c in enumerate(coefs):
            up = c * unscale
            out[k] = SHIFT * up if out[k] is None else out[k] + SHIFT * up
            out[k + 1] = up
        return out

    def inner(a, b):
        rows = []
        for i, x in enumerate(a):
            rows.append(x * sum(gram[i, j] * y for j, y in enumerate(b)))
        return sum(rows)

    def plus(a, factor, b):
        out = list(a) + [None] * (len(b) - len(a))
        for k, y in enumerate(b):
            out[k] = factor * y if out[k] is None else out[k] + factor * y
        return out

    residual = [one]
    field = []
    image = image_of(residual)
    norm = inner(residual, residual)
    step = norm / inner(residual, image)
    direction, along = residual, image
    for k in range(ITERS):
        field = plus(field, step, direction)
        residual = plus(residual, -step, along)
        if k + 1 < ITERS:
            image = image_of(residual)
            following = inner(residual, residual)
            product = inner(residual, image)
            ratio = following / norm
            step = following / (product - ratio * following / step)
            direction = plus(residual, ratio, direction)
            along = plus(image, ratio, along)
            norm = following
    basis = [ref[...] for ref in basis_refs]
    solution_ref[...] = sum(c * v for c, v in zip(field, basis))
    residual_ref[...] = sum(c * v for c, v in zip(residual, basis))


def params(mib):
    return pltpu.CompilerParams(vmem_limit_bytes=mib * 1024 * 1024)


def vmem(count):
    return [pl.BlockSpec(memory_space=pltpu.VMEM)] * count


def shape(dims, dtype=F32):
    return jax.ShapeDtypeStruct(dims, dtype)


def per_device(
    right_side, diag_shift, dictionary, diag_ids, diag_gain, cycle_ids, cycle_weights,
    link_rows, link_ids, link_weights, *, devices,
):
    nb = diag_ids.shape[0]
    blocks, width, _ = dictionary.shape
    _, levels, half = link_rows.shape
    bits = devices.bit_length() - 1
    masks = [2 ** (bits - 1 - level) for level in range(levels)]
    merged = masks.index(1) if 1 in masks else -1
    links = levels * half
    used = 2 * nb + links + 1
    entries = -(-used // 128) * 128
    sources = -(-(nb + links + 16) // 128) * 128
    assert sources <= 512 and nb <= 256
    extra = -(-(used // SLOT) // (GROUP // SLOT))
    groups = blocks * SLOT // GROUP + extra

    sure = blocks * SLOT // GROUP + 1
    parity = (lax.axis_index("rows") & 1).astype(jnp.int32)[None]
    first = right_side.reshape(nb, width)
    shifts = diag_shift.reshape(nb, width)

    small = [first, diag_ids[None], diag_gain[None], cycle_ids.T, cycle_weights.T]
    small += [jnp.swapaxes(array, 0, 1) for array in (link_rows, link_ids, link_weights)]
    send_shapes = [shape((half + 8 * (level == merged), width)) for level in range(levels)]
    edge_shape = shape((8, width))
    outs = pl.pallas_call(
        functools.partial(
            prepare, nb=nb, blocks=blocks, levels=levels, half=half, merged=merged, groups=groups, sure=sure,
            entries=entries, sources=sources,
        ),
        out_shape=send_shapes
        + [
            edge_shape,
            shape((links, nb), BF16),
            shape((groups * GROUP, sources), BF16),
            shape((2 * nb, groups * GROUP), BF16),
            shape((1, 128), jnp.int32),
        ],
        in_specs=[pl.BlockSpec(memory_space=pltpu.SMEM)] + [pl.BlockSpec(memory_space=pltpu.HBM)] * 8,
        out_specs=vmem(levels + 5),
        scratch_shapes=[
            pltpu.VMEM((128, entries), BF16),
            *(pltpu.VMEM(array.shape, array.dtype) for array in small),
            pltpu.SemaphoreType.DMA((len(small),)),
        ],
        compiler_params=params(24),
        cost_estimate=pl.CostEstimate(flops=COST, bytes_accessed=0, transcendentals=0),
        name="prepare",
)(parity, *(pltpu.with_memory_space_constraint(array, pltpu.HBM) for array in small))
    sends, (edge, select, gather, scatter, table) = outs[:levels], outs[levels:]

    def exchange(sends, edge):
        near = [(i, i ^ 1) for i in range(devices)]
        far = [(i, (i + 1) % devices if i % 2 else (i - 1) % devices) for i in range(devices)]
        edges = lax.ppermute(edge, "rows", far)
        if merged < 0:
            edges = jnp.concatenate([edges, lax.ppermute(edge, "rows", near)], axis=0)
        got = []
        for level in range(levels):
            pairs = [(i, i ^ masks[level]) for i in range(devices)]
            got.append(lax.ppermute(sends[level], "rows", pairs))
        return got, edges

    scratch = [
        pltpu.VMEM((sources, 2 * width), BF16),
        pltpu.VMEM((2 * sure * GROUP, width), BF16),
        pltpu.VMEM((sure * GROUP, 2 * width), BF16),
        pltpu.SMEM((1, 128), jnp.int32),
        pltpu.SemaphoreType.DMA,
    ]
    basis = [first]
    for k in range(ITERS):
        got, edges = exchange(sends, edge)
        common = dict(levels=levels, half=half, merged=merged, sure=sure)
        if k == 0:
            following, *outs = pl.pallas_call(
                functools.partial(first_kernel, **common),
                out_shape=[shape((nb, width))] + send_shapes
                + [edge_shape, shape((blocks, width, 2 * width), BF16), shape((1, 128))],
                in_specs=vmem(8 + levels),
                out_specs=vmem(levels + 4),
                scratch_shapes=scratch,
                compiler_params=params(24),
                name="first",
            )(table, first, shifts, *got, edges, select, gather, scatter, dictionary)
            sends, (edge, wide, scale) = outs[:levels], outs[levels:]
        elif k + 1 < ITERS:
            following, *outs = pl.pallas_call(
                functools.partial(step_kernel, **common),
                out_shape=[shape((nb, width))] + send_shapes + [edge_shape],
                in_specs=vmem(9 + levels),
                out_specs=vmem(levels + 2),
                scratch_shapes=scratch,
                compiler_params=params(24),
                name="step",
            )(table, basis[-1], shifts, scale, *got, edges, select, gather, scatter, wide)
            sends, edge = outs[:levels], outs[levels]
        else:
            following, sums = pl.pallas_call(
                functools.partial(last_kernel, **common),
                out_shape=[shape((nb, width)), shape((devices, 128))],
                in_specs=vmem(8 + levels + ITERS - 1),
                out_specs=vmem(2),
                scratch_shapes=scratch,
                compiler_params=params(24),
                name="last",
            )(table, basis[-1], shifts, scale, *got, edges, gather, scatter, wide, *basis[:-1])
        basis.append(following)
    sums = lax.all_to_all(sums, "rows", 0, 0, tiled=True)
    field, residual = pl.pallas_call(
        finish,
        out_shape=[shape((nb, width))] * 2,
        in_specs=vmem(2 + len(basis)),
        out_specs=vmem(2),
        compiler_params=params(8),
        name="finish",
    )(sums, scale, *basis)
    return field.reshape(-1), residual.reshape(-1)


def solution(mesh):
    placed = (
        P("rows"), P("rows"), P(), P("rows"), P("rows"), P("rows", None), P("rows", None),
        P("rows", None, None), P("rows", None, None), P("rows", None, None),
    )
    return jax.shard_map(
        functools.partial(per_device, devices=mesh.shape["rows"]),
        mesh=mesh, in_specs=placed, out_specs=(P("rows"), P("rows")), check_vma=False,
    )
```
